32 devices in a mesh: slides: 2 (over y), seq: 4 (over z), sub: 4 (over x, core).
Axes of the slice: x: 2, y: 2, z: 4, core: 2. Of those that a mesh axis runs over, the one named last changes fastest.
Arguments:
- q_heads: bfloat16 [8192, 768], P(('slides', 'seq'), 'sub'), parts along dimension 0, may hold values from -8 to 8
- k_heads: bfloat16 [8192, 768], P(('slides', 'seq'), 'sub'), parts along dimension 0, may hold values from -8 to 8
- v_heads: bfloat16 [8192, 768], P(('slides', 'seq'), 'sub'), parts along dimension 0, may hold values from -6 to 6
- w_out: bfloat16 [768, 768], replicated, may hold values from -0.21875 to 0.21875
- offsets: int32 [2, 16], replicated, may hold values from 0 to 15, as said below
- valid: int32 [2], P('slides'), parts along dimension 0, may hold values from 3073 to 4096
Outputs:
- mixed: bfloat16 [8192, 768], P(('slides', 'seq'), 'sub'), parts along dimension 0
The draws below stay inside these ranges and needn't reach their ends.
There are 2 independent parts, one for each index of `slides`. The reference program is written for one: setup_inputs(seed, part) draws one part's arguments, and reference() takes and returns one part's arrays. A program takes and returns all parts, laid end to end along the dimension named above; an argument that names none is the same for every part. Nothing has to cross between parts.
Inputs may be any that keep to these rules, and one draw needn't show every extreme that they name: `offsets`: row 0 lies below 4, row 1 below 16. Tiles at positions valid[0] and beyond are padding.
All inputs are finite; a program needn't handle non-finite values.
Results may differ from the reference program's by a relative error of at most 0.012.
Values may be sent and summed in bfloat16 or wider, within the bound.
A program may use at most 64 MiB of HBM per device.

```python
import jax
import jax.numpy as jnp
from jax import lax

D = 768
H = 16
HS = 48
TOK_DEV = 1024
GROUP = 4
R1 = 4
R2 = 16
TOKENS = 4096


def paired_fields(key):
    first_key = jax.random.fold_in(key, 101)
    second_key = jax.random.fold_in(key, 202)
    query = jnp.clip(2.0 * jax.random.normal(first_key, (TOKENS, D), jnp.float32), -8.0, 8.0)
    key_out = jnp.clip(2.0 * jax.random.normal(second_key, (TOKENS, D), jnp.float32), -8.0, 8.0)
    return (query, key_out)


def draw_q_heads(key, part):
    return paired_fields(key)[0].astype(jnp.bfloat16)


def draw_k_heads(key, part):
    return paired_fields(key)[1].astype(jnp.bfloat16)


def draw_offsets(key, part):
    middle = jax.random.randint(jax.random.fold_in(key, 7), (H,), 0, R1).astype(jnp.int32)
    widest = jax.random.randint(jax.random.fold_in(key, 8), (H,), 0, R2).astype(jnp.int32)
    low_head = jax.random.randint(jax.random.fold_in(key, 9), (), 0, H)
    high_head = jax.random.randint(jax.random.fold_in(key, 10), (), 0, H)
    top_head = jax.random.randint(jax.random.fold_in(key, 11), (), 0, H)
    middle = middle.at[low_head].set(0)
    middle = middle.at[(low_head + 1 + top_head % (H - 1)) % H].set(R1 - 1)
    widest = widest.at[high_head].set(R2 - 1)
    return jnp.stack([middle, widest], axis=0).astype(jnp.int32)


def shard_levels(own_key, extent, shards, least, top_value):
    level, own = 1.0, jax.random.fold_in(own_key, 6)
    for axis_at, shards_of in shards:
        steps = jnp.exp(jax.random.uniform(jax.random.fold_in(own, axis_at), (shards_of,), jnp.float32, least / len(shards), top_value / len(shards)))
        level = level * jnp.repeat(steps, extent[axis_at] // shards_of).reshape([-1 if axis == axis_at else 1 for axis in range(len(extent))])
    return level


def noise(key, dims, width, most, cuts=(), kind=jnp.bfloat16):
    values = width * jax.random.normal(key, dims, jnp.float32)
    if cuts:
        values = values * shard_levels(key, dims, cuts, -0.22, 0.18)
    return jnp.clip(values, -most, most).astype(kind)


def setup_inputs(seed: int = 0, part: int = 0) -> dict:
    keys = jax.random.split(jax.random.key(seed), 7)
    own_keys = jax.random.split(jax.random.fold_in(keys[6], part), 7)
    q_heads = draw_q_heads(jax.random.fold_in(jax.random.fold_in(keys[6], part), 71), part)
    k_heads = draw_k_heads(jax.random.fold_in(jax.random.fold_in(keys[6], part), 71), part)
    v_heads = noise(own_keys[2], (TOKENS, D), 1.0, 6.0, ((0, 4), (1, 4)))
    w_out = noise(keys[3], (D, D), D ** -0.5, 0.21875)
    offsets = draw_offsets(jax.random.fold_in(keys[6], 71), part)
    valid = jax.random.randint(own_keys[5], (1,), TOKENS - TOK_DEV + 1, TOKENS + 1).astype(jnp.int32)
    return dict(q_heads=q_heads, k_heads=k_heads, v_heads=v_heads, w_out=w_out, offsets=offsets, valid=valid)


NEG_FILL = -1.0e30


def pick_rows(source, stride, chosen):
    grouped = source.reshape(source.shape[0] // stride, stride, source.shape[1], source.shape[2])
    onehot = jnp.arange(stride, dtype=jnp.int32)[:, None] == chosen[None, :]
    return jnp.sum(jnp.where(onehot[None, :, :, None], grouped, jnp.zeros((), source.dtype)), axis=1)


def spread_back(maxima, totals, numer, stride, chosen):
    onehot = (jnp.arange(stride, dtype=jnp.int32)[:, None] == chosen[None, :])[None]
    count = maxima.shape[0] * stride
    full_max = jnp.where(onehot, maxima[:, None, :], NEG_FILL).reshape(count, maxima.shape[1])
    full_tot = jnp.where(onehot, totals[:, None, :], 0.0).reshape(count, maxima.shape[1])
    full_num = jnp.where(onehot[..., None], numer[:, None, :, :], 0.0).reshape(count, numer.shape[1], numer.shape[2])
    return full_max, full_tot, full_num


def one_branch(query, key_in, value, seg_len, stride, chosen, limit):
    total_rows = query.shape[0]
    heads = query.shape[1]
    q_sel = pick_rows(query, stride, chosen)
    k_sel = pick_rows(key_in, stride, chosen)
    v_sel = pick_rows(value, stride, chosen)
    per_seg = seg_len // stride
    n_segs = total_rows // seg_len
    positions = jnp.arange(total_rows // stride, dtype=jnp.int32)[:, None] * stride + chosen[None, :]
    live = positions < limit

    def arrange(block):
        moved = jnp.moveaxis(block, 1, 0)
        return moved.reshape((heads * n_segs, per_seg) + moved.shape[2:])

    def attend(items):
        q_blk, k_blk, v_blk, l_blk = items
        scores = jnp.dot(q_blk, k_blk.T, preferred_element_type=jnp.float32) * (HS ** -0.5)
        scores = jnp.where(l_blk[None, :], scores, NEG_FILL)
        peak = jnp.max(scores, axis=1)
        probs = jnp.exp(scores - peak[:, None])
        mass = jnp.sum(probs, axis=1)
        numer = jnp.dot(probs.astype(jnp.bfloat16), v_blk, preferred_element_type=jnp.float32)
        return peak, mass, numer

    peak, mass, numer = lax.map(attend, (arrange(q_sel), arrange(k_sel), arrange(v_sel), arrange(live)))
    peak = peak.reshape(heads, total_rows // stride).T
    mass = mass.reshape(heads, total_rows // stride).T
    numer = jnp.moveaxis(numer.reshape(heads, total_rows // stride, HS), 0, 1)
    return spread_back(peak, mass, numer, stride, chosen)


def reference(q_heads, k_heads, v_heads, w_out, offsets, valid):
    total_rows = q_heads.shape[0]
    query = q_heads.reshape(total_rows, H, HS)
    key_in = k_heads.reshape(total_rows, H, HS)
    value = v_heads.reshape(total_rows, H, HS)
    limit = valid[0]
    zero_offs = jnp.zeros((H,), jnp.int32)
    branches = [
        one_branch(query, key_in, value, TOK_DEV, 1, zero_offs, limit),
        one_branch(query, key_in, value, GROUP * TOK_DEV, R1, offsets[0], limit),
        one_branch(query, key_in, value, TOKENS, R2, offsets[1], limit),
    ]
    top = jnp.maximum(jnp.maximum(branches[0][0], branches[1][0]), branches[2][0])
    denom = jnp.zeros_like(top)
    numer = jnp.zeros_like(branches[0][2])
    for peak, mass, partial_num in branches:
        weight = jnp.exp(peak - top)
        denom = denom + weight * mass
        numer = numer + weight[..., None] * partial_num
    attn = (numer / denom[..., None]).reshape(total_rows, D).astype(jnp.bfloat16)
    projected = jnp.dot(attn, w_out, preferred_element_type=jnp.float32)
    keep = jnp.arange(total_rows, dtype=jnp.int32) < limit
    return jnp.where(keep[:, None], projected, 0.0).astype(jnp.bfloat16)
```

```python
import functools

import jax
import jax.numpy as jnp
from jax import lax
from jax.experimental import pallas as pl
from jax.experimental.pallas import tpu as pltpu
from jax.sharding import PartitionSpec as P

HS = 48
FP = 64
GROUP = 4
R1 = 4
R2 = 16
LANES = 128
HALF = 64
MASKED = -1e30
MESH = pl.DeviceIdType.MESH
EXP_SCALE = HS ** (-0.5) * 1.4426950408889634
LOG2E = 1.4426950408889634
CONTRACT_LAST = (((1,), (1,)), ((), ()))
BF, F32, I32 = jnp.bfloat16, jnp.float32, jnp.int32


def iota(shape, dim):
    return lax.broadcasted_iota(I32, shape, dim)


def mm(a, b):
    return jnp.dot(a, b, preferred_element_type=F32)


def mm_t(a, b):
    return lax.dot_general(a, b, CONTRACT_LAST, preferred_element_type=F32)


def combine(parts):
    top = functools.reduce(jnp.maximum, [lse for _, lse in parts])
    weights = [jnp.exp2(lse - top) for _, lse in parts]
    scale = 1.0 / functools.reduce(jnp.add, weights)
    return functools.reduce(jnp.add, [o * (w * scale) for (o, _), w in zip(parts, weights)])


def kernel(
    n_seq, n_sub, heads,
    q_hbm, k_hbm, v_hbm, w_hbm, off_hbm, valid_hbm, o_ref,
    off_ref, valid_ref,
    q_ref, k_aug, v_aug, w_ref, wt,
    perm, sel, kr, pq, pk, pv, wide, mid,
    scores, near_o, near_l, mid_o, mid_m, spread, xg,
    wide_send, wide_recv, mid_send, mid_recv, x_send, x_recv, in_sem,
):
    cols, rows = q_ref.shape
    phase = rows // R1
    strip = rows // R2
    square = 2 * LANES
    seq = lax.axis_index("seq")
    sub = lax.axis_index("sub")
    pos = lax.rem(seq, GROUP)
    group0 = seq - pos
    has_left = pos > 0
    has_right = pos < GROUP - 1
    bits = [1 << b for b in reversed(range(n_sub.bit_length() - 1))]

    small = [
        pltpu.make_async_copy(off_hbm, off_ref, in_sem.at[2 * heads + 2]),
        pltpu.make_async_copy(valid_hbm, valid_ref, in_sem.at[2 * heads + 3]),
    ]
    fetches = []
    for src, dst in ((k_hbm, k_aug), (v_hbm, v_aug)):
        for h in range(heads):
            fetches.append((src.at[pl.ds(h * HS, HS), :], dst.at[pl.ds(h * FP, HS), :]))
    fetches += [(q_hbm, q_ref), (w_hbm, w_ref)]
    fetches = [
        pltpu.make_async_copy(src, dst, in_sem.at[i]) for i, (src, dst) in enumerate(fetches)
    ]
    for fetch in small + fetches:
        fetch.start()
    barrier = pltpu.get_barrier_semaphore()
    for step, there in ((1, seq < n_seq - 1), (-1, seq > 0)):
        @pl.when(there)
        def _():
            pl.semaphore_signal(
                barrier, inc=1, device_id={"seq": seq + step}, device_id_type=MESH
            )
    for bit in bits:
        pl.semaphore_signal(barrier, inc=1, device_id={"sub": sub ^ bit}, device_id_type=MESH)

    low = iota((1, LANES), 1) < HALF
    block0 = seq * rows

    def plan(head):
        o0, o1 = off_ref[0, head], off_ref[1, head]
        m1 = lax.rem(o1, R1)
        late = o0
        second = jnp.where(m1 == o0, lax.rem(o0 + 1, R1), m1)
        third = 0
        for m in reversed(range(R1 - 1)):
            third = jnp.where((late != m) & (second != m), m, third)
        return o0, m1, lax.div(o1, R1), (late, second, third, 6 - late - second - third)

    with jax.named_scope("consts"):
        tok, at = iota((square, square), 0), iota((square, square), 1)
        for odd in range(2):
            hit = tok == at % HALF * R1 + ((at // HALF) ^ odd)
            perm[odd] = jnp.where(hit, 1.0, 0.0).astype(BF)
        at_l, at_j = iota((square, LANES), 0), iota((square, LANES), 1)
        for a in range(R1):
            for half in range(2):
                hit = at_l == (at_j - half * HALF) * R1 + a
                sel[a, pl.ds(half * square, square), :] = jnp.where(hit, 1.0, 0.0).astype(BF)
        for fetch in small:
            fetch.wait()
        limit = valid_ref[0]
        plans = [plan(sub * heads + h) for h in range(heads)]
        tail_one = jnp.where(iota((FP - HS, square), 0) == 0, 1.0, 0.0).astype(BF)
        for h in range(heads):
            tail = pl.ds(h * FP + HS, FP - HS)
            for m in range(R1):
                pq[m, tail, :] = tail_one
            place = block0 + iota((FP - HS, rows), 1)
            first = iota((FP - HS, rows), 0) == 0
            v_aug[tail, :] = jnp.where(first, 1.0, 0.0).astype(BF)
            k_aug[tail, :] = jnp.where(first & (place >= limit), MASKED, 0.0).astype(BF)

    def permuted(lhs_of, store):
        for c in range(rows // (2 * square)):
            outs = [
                mm(lhs_of(pl.ds((2 * c + b) * square, square)), perm[b]) for b in range(2)
            ]
            for m in range(R1):
                half = slice((m // 2) * LANES, (m // 2 + 1) * LANES)
                even, odd = outs[0][:, half], outs[1][:, half]
                if m % 2:
                    even, odd = odd, even
                store(m, slice(c * LANES, (c + 1) * LANES), jnp.where(low, even, odd).astype(BF))

    with jax.named_scope("load"):
        for fetch in fetches[:2 * heads]:
            fetch.wait()

        def store_kv(m, lanes, val):
            pk[m, :, lanes] = val[:cols]
            pv[m, :, lanes] = val[cols:]

        permuted(
            lambda t: jnp.concatenate(
                [ref[pl.ds(h * FP, HS), t] for ref in (k_aug, v_aug) for h in range(heads)], axis=0
            ),
            store_kv,
        )
        for h in range(heads):
            o0, m1, a, _ = plans[h]
            feat = pl.ds(h * HS, HS)
            mid[pos, h // 2, pl.ds((h % 2) * 2 * HS, HS), :] = pk[o0, feat, :]
            mid[pos, h // 2, pl.ds((h % 2) * 2 * HS + HS, HS), :] = pv[o0, feat, :]
            both = jnp.concatenate([pk[m1, feat, :], pv[m1, feat, :]], axis=1)
            wide[seq, feat, :] = mm(both, sel[a]).astype(BF)

    with jax.named_scope("barrier"):
        inner = (seq > 0) & (seq < n_seq - 1)

        @pl.when(inner)
        def _():
            pl.semaphore_wait(barrier, len(bits) + 2)

        @pl.when(jnp.logical_not(inner))
        def _():
            pl.semaphore_wait(barrier, len(bits) + 1)

    def wide_copy(origin, rightward):
        target = seq + 1 if rightward else seq - 1
        return pltpu.make_async_remote_copy(
            src_ref=wide.at[origin], dst_ref=wide.at[origin],
            send_sem=wide_send.at[0 if rightward else 1, origin], recv_sem=wide_recv.at[origin],
            device_id={"seq": target}, device_id_type=MESH,
        )

    @pl.when(seq < n_seq - 1)
    def _():
        wide_copy(seq, True).start()

    @pl.when(seq > 0)
    def _():
        wide_copy(seq, False).start()

    def wide_relay(dist):
        @pl.when(seq - dist >= 0)
        def _():
            wide_copy(seq - dist, True).wait_recv()

            @pl.when(seq < n_seq - 1)
            def _():
                wide_copy(seq - dist, True).start()

        @pl.when(seq + dist < n_seq)
        def _():
            wide_copy(seq + dist, False).wait_recv()

            @pl.when(seq > 0)
            def _():
                wide_copy(seq + dist, False).start()

    def mid_copy(origin, chunk, rightward):
        way = 0 if rightward else 1
        target = seq + 1 if rightward else seq - 1
        return pltpu.make_async_remote_copy(
            src_ref=mid.at[origin, chunk], dst_ref=mid.at[origin, chunk],
            send_sem=mid_send.at[way, origin, chunk], recv_sem=mid_recv.at[origin, chunk],
            device_id={"seq": target}, device_id_type=MESH,
        )

    @pl.when(has_right)
    def _():
        mid_copy(pos, 0, True).start()

    @pl.when(has_left)
    def _():
        mid_copy(pos, 0, False).start()

    def relay(dist, chunk):
        @pl.when(pos - dist >= 0)
        def _():
            mid_copy(pos - dist, chunk, True).wait_recv()

            @pl.when(has_right)
            def _():
                mid_copy(pos - dist, chunk, True).start()

        @pl.when(pos + dist < GROUP)
        def _():
            mid_copy(pos + dist, chunk, False).wait_recv()

            @pl.when(has_left)
            def _():
                mid_copy(pos + dist, chunk, False).start()

    def x_ref(block, slab):
        if slab in (0, R1):
            return xg.at[block, 0, pl.ds((slab // R1) * (cols // 2), cols // 2)]
        return xg.at[block, slab]

    def x_copy(at_bit, held, slab):
        bit = bits[at_bit]
        ref = x_ref(sub ^ held, slab)
        return pltpu.make_async_remote_copy(
            src_ref=ref, dst_ref=ref,
            send_sem=x_send.at[at_bit, held, slab], recv_sem=x_recv.at[held ^ bit, slab],
            device_id={"sub": sub ^ bit}, device_id_type=MESH,
        )

    def x_plan():
        held, todo = [0], []
        for at_bit, bit in enumerate(bits):
            todo += [(at_bit, x) for x in held]
            held = held + [x ^ bit for x in held]
        return todo

    def x_start(slab):
        for at_bit, x in x_plan():
            if x == 0:
                x_copy(at_bit, x, slab).start()

    def x_recv_wait(block, slab):
        ref = x_ref(sub ^ block, slab)
        pltpu.make_async_remote_copy(
            src_ref=ref, dst_ref=ref,
            send_sem=x_send.at[0, 0, slab], recv_sem=x_recv.at[block, slab],
            device_id={"sub": sub ^ block}, device_id_type=MESH,
        ).wait_recv()

    def x_forward(slab):
        waited = set()
        for at_bit, x in x_plan():
            if x:
                if x not in waited:
                    waited.add(x)
                    x_recv_wait(x, slab)
                x_copy(at_bit, x, slab).start()
        return waited

    with jax.named_scope("prep"):
        fetches[2 * heads].wait()

        def store_q(m, lanes, val):
            for h in range(heads):
                pq[m, pl.ds(h * FP, HS), lanes] = val[h * HS:(h + 1) * HS]

        permuted(lambda t: q_ref[:, t], store_q)
        for h in range(heads):
            kr[h] = k_aug[pl.ds(h * FP, FP), :].T

    def attend(keys, values, queries, before=None):
        scores = mm(keys, queries)
        peak = jnp.max(scores, axis=0, keepdims=True)
        if before is not None:
            peak = jnp.maximum(peak, before)
        probs = jnp.exp2((scores - peak) * EXP_SCALE).astype(BF)
        return peak, mm(values, probs)

    def finish(peak, out):
        mass = out[HS:HS + 1]
        return out[:HS] * (1.0 / mass), peak * EXP_SCALE + jnp.log(mass) * LOG2E

    pieces = rows // phase

    def score_piece(to, h, m, c, peak):
        keys = kr[h, pl.ds(c * phase, phase), :]
        part = mm(keys, pq[m, pl.ds(h * FP, FP), :])
        scores[to, pl.ds(c * phase, phase), :] = part
        top = jnp.max(part, axis=0, keepdims=True)
        return top if peak is None else jnp.maximum(peak, top)

    combos = [(m, h) for m in range(R1) for h in range(heads)]

    def mid_start(chunk):
        @pl.when(has_right)
        def _():
            mid_copy(pos, chunk, True).start()

        @pl.when(has_left)
        def _():
            mid_copy(pos, chunk, False).start()

    def near_step(i, peak):
        m, h = combos[i]
        ahead = acc = None
        for c in range(pieces):
            if i + 1 < len(combos):
                m_next, h_next = combos[i + 1]
                ahead = score_piece((i + 1) % 2, h_next, m_next, c, ahead)
            part = scores[i % 2, pl.ds(c * phase, phase), :]
            probs = jnp.exp2((part - peak) * EXP_SCALE).astype(BF)
            out = mm(v_aug[pl.ds(h * FP, FP), pl.ds(c * phase, phase)], probs)
            acc = out if acc is None else acc + out
        out, lse = finish(peak, acc)
        near_o[m, pl.ds(h * HS, HS), :] = out
        near_l[m, pl.ds(h, 1), :] = lse
        return ahead

    with jax.named_scope("near"):
        peak = None
        for c in range(pieces):
            peak = score_piece(0, 0, 0, c, peak)
        for i in range(len(combos)):
            peak = near_step(i, peak)
            if i == 6:
                wide_relay(1)
                mid_start(1)
            if i == 12:
                relay(1, 0)

    def ship(slab, h, val):
        xg[sub, slab, pl.ds(h * HS, HS), :] = val.astype(BF)

    with jax.named_scope("ship_near"):
        for slab in (2, 3):
            for h in range(heads):
                ship(slab, h, near_o[plans[h][3][slab], pl.ds(h * HS, HS), :])
            x_start(slab)

    ones_tail = jnp.where(iota((FP - HS, phase), 0) == 0, 1.0, 0.0).astype(BF)

    def mid_step(origin, chunk, first):
        pair = range(chunk * 2, chunk * 2 + 2)
        lane = iota((FP - HS, phase), 1)
        top_row = iota((FP - HS, phase), 0) == 0
        scored, vals, fore = [], [], []
        for h in pair:
            o0 = plans[h][0]
            at = jnp.where(lax.rem(o0, 2) == 1, lane ^ HALF, lane)
            place = (group0 + origin) * rows + at * R1 + o0
            dead = jnp.where(top_row & (place >= limit), MASKED, 0.0).astype(BF)
            k_at, v_at = [pl.ds((h % 2) * 2 * HS + i * HS, HS) for i in range(2)]
            k_t = jnp.concatenate([mid[origin, chunk, k_at, :], dead], axis=0)
            vals.append(jnp.concatenate([mid[origin, chunk, v_at, :], ones_tail], axis=0))
            scored.append(mm(k_t.T, pq[o0, pl.ds(h * FP, FP), :]))
            fore.append(None if first else (mid_m[pl.ds(h, 1), :], mid_o[pl.ds(h * FP, FP), :]))
        done = []
        for score, val, before in zip(scored, vals, fore):
            peak = jnp.max(score, axis=0, keepdims=True)
            if before is not None:
                peak = jnp.maximum(peak, before[0])
            probs = jnp.exp2((score - peak) * EXP_SCALE).astype(BF)
            done.append((peak, mm(val, probs)))
        for i, h in enumerate(pair):
            peak, out = done[i]
            if not first:
                out = out + fore[i][1] * jnp.exp2((fore[i][0] - peak) * EXP_SCALE)
            done[i] = (peak, out)
            mid_m[pl.ds(h, 1), :] = peak
            mid_o[pl.ds(h * FP, FP), :] = out
        return done

    partner = pos ^ 1
    second = 2 - lax.div(pos, 2)
    third = 3 - 3 * lax.div(pos, 2)

    with jax.named_scope("mid_own"):
        mid_step(pos, 0, True)
    with jax.named_scope("wide_relay2"):
        wide_relay(2)
    with jax.named_scope("mid_1"):
        mid_step(pos, 1, True)
        mid_step(partner, 0, False)
    with jax.named_scope("relay11"):
        relay(1, 1)
    with jax.named_scope("mid_1b"):
        mid_step(partner, 1, False)
    with jax.named_scope("weights"):
        fetches[2 * heads + 1].wait()
        for s in range(n_sub):
            @pl.when(sub == s)
            def _():
                wt[...] = w_ref[:, s * cols:(s + 1) * cols].T
    with jax.named_scope("relay20"):
        relay(2, 0)
    with jax.named_scope("mid_2"):
        mid_step(second, 0, False)
    with jax.named_scope("x_fwd2"):
        waited = {2: x_forward(2)}
    with jax.named_scope("wide_relay3"):
        for dist in range(3, n_seq):
            wide_relay(dist)

    with jax.named_scope("wide"):
        q_rows = []
        for h in range(heads):
            _, m1, a, _ = plans[h]
            q_h = mm(pq[m1, pl.ds(h * FP, FP), :], sel[a, pl.ds((h % 2) * square, square), :])
            zero = jnp.zeros((FP, LANES), BF)
            q_h = q_h.astype(BF)
            q_rows.append(jnp.concatenate([q_h, zero] if h < 2 else [zero, q_h], axis=1))
        q_wide = jnp.concatenate(q_rows, axis=0)
        keys, values = [], []
        zeros_tail = jnp.zeros((FP - HS - 8, LANES), F32)
        for pr in range(n_seq // 2):
            one, two = [wide[2 * pr + i].astype(F32) for i in range(2)]
            k_pair = jnp.where(low, one, pltpu.roll(two, HALF, 1))
            v_pair = jnp.where(low, pltpu.roll(one, HALF, 1), two)
            k_rows, v_rows = [], []
            for h in range(heads):
                _, m1, a, _ = plans[h]
                lane = iota((FP - HS, LANES), 1)
                row0 = iota((FP - HS, LANES), 0) == 0
                at = lane % HALF * R1 + a
                at = jnp.where(lax.rem(m1, 2) == 1, at ^ HALF, at)
                place = (2 * pr + lane // HALF) * rows + at * R1 + m1
                k_rows += [
                    k_pair[h * HS:(h + 1) * HS],
                    jnp.where(row0 & (place >= limit), MASKED, 0.0),
                ]
                v_rows += [v_pair[h * HS:(h + 1) * HS], jnp.where(row0, 1.0, 0.0)]
            keys.append(jnp.concatenate(k_rows, axis=0).astype(BF).T)
            values.append(jnp.concatenate(v_rows, axis=0).astype(BF))
        peak, out = attend(
            jnp.concatenate(keys, axis=0), jnp.concatenate(values, axis=1), q_wide
        )
        for h in range(heads):
            _, m1, a, _ = plans[h]
            col = slice((h // 2) * LANES, (h // 2 + 1) * LANES)
            o_h, lse = finish(peak[:, col], out[h * FP:(h + 1) * FP, col])
            top = jnp.floor(lse * 0.25) * 4.0
            rest = lse - top
            middle = jnp.floor(rest * 64.0) * (1.0 / 64.0)
            r = iota((FP - HS, LANES), 0)
            tail = jnp.where(r == 0, top, jnp.where(r == 1, middle, jnp.where(r == 2, rest - middle, jnp.where(r == 3, 1.0, 0.0))))
            z = jnp.concatenate([o_h, tail], axis=0).astype(BF)
            put = mm_t(z, sel[a, pl.ds((h % 2) * square, square), :])
            spread[pl.ds(h * FP, HS), :] = put[:HS]
            lse = put[HS:HS + 1] + put[HS + 1:HS + 2] + put[HS + 2:HS + 3]
            lse = jnp.where(put[HS + 3:HS + 4] > 0.5, lse, MASKED)
            spread[pl.ds(h * FP + HS, 8), :] = jnp.broadcast_to(lse, (8, phase))
            two = plans[h][3][1]
            feat = pl.ds(h * HS, HS)
            lse = jnp.where(two == m1, lse, MASKED)
            ship(1, h, combine([
                (near_o[two, feat, :], near_l[two, pl.ds(h, 1), :]), (put[:HS], lse),
            ]))
        x_start(1)

    with jax.named_scope("relay21"):
        relay(2, 1)
    with jax.named_scope("mid_2b"):
        mid_step(second, 1, False)
    with jax.named_scope("x_fwd3"):
        waited[3] = x_forward(3)

    for chunk in range(2):
        with jax.named_scope("relay3"):
            relay(3, chunk)
        with jax.named_scope("mid_3"):
            done = mid_step(third, chunk, False)
            for h in range(chunk * 2, chunk * 2 + 2):
                o0, m1 = plans[h][:2]
                feat = pl.ds(h * HS, HS)
                lse_w = spread[pl.ds(h * FP + HS, 1), :]
                ship(0, h, combine([
                    (near_o[o0, feat, :], near_l[o0, pl.ds(h, 1), :]),
                    finish(*done[h % 2]),
                    (spread[pl.ds(h * FP, HS), :], jnp.where(m1 == o0, lse_w, MASKED)),
                ]))
            x_start(chunk * R1)
        if chunk == 0:
            with jax.named_scope("x_fwd1"):
                waited[1] = x_forward(1)

    with jax.named_scope("x_wait"):
        for slab in (0, R1):
            waited[slab] = x_forward(slab)
        for slab in (2, 3, 1, 0, R1):
            for x in range(1, n_sub):
                if x not in waited[slab]:
                    x_recv_wait(x, slab)

    with jax.named_scope("project"):
        outs = []
        every = [plan(i)[3] for i in range(n_sub * heads)]
        for m in range(R1):
            parts = []
            for d in range(n_sub):
                for h in range(heads):
                    order = every[d * heads + h]
                    slab = 3
                    for s in range(3):
                        slab = jnp.where(order[s] == m, s, slab)
                    parts.append(xg[d, slab, pl.ds(h * HS, HS), :])
            outs.append(mm(wt[...], jnp.concatenate(parts, axis=0)).astype(BF).astype(F32))
        for c in range(rows // (2 * square)):
            at = slice(c * LANES, (c + 1) * LANES)
            for odd in range(2):
                pieces = [
                    jnp.where(low, outs[2 * i + odd][:, at], outs[2 * i + 1 - odd][:, at])
                    for i in range(2)
                ]
                res = mm_t(jnp.concatenate(pieces, axis=1).astype(BF), perm[odd])
                first = (2 * c + odd) * square
                place = block0 + first + iota((1, square), 1)
                o_ref[:, first:first + square] = jnp.where(place < limit, res, 0.0).astype(BF)

    with jax.named_scope("drain"):
        for o in range(n_seq):
            @pl.when((seq < n_seq - 1) & (seq >= o))
            def _():
                wide_copy(o, True).wait_send()

            @pl.when((seq > 0) & (seq <= o))
            def _():
                wide_copy(o, False).wait_send()
        for chunk in range(2):
            for o in range(GROUP):
                @pl.when(has_right & (pos >= o))
                def _():
                    mid_copy(o, chunk, True).wait_send()

                @pl.when(has_left & (pos <= o))
                def _():
                    mid_copy(o, chunk, False).wait_send()
        for slab in range(R1 + 1):
            for at_bit, x in x_plan():
                x_copy(at_bit, x, slab).wait_send()


def local(n_seq, n_sub, q_heads, k_heads, v_heads, w_out, offsets, valid):
    rows, cols = q_heads.shape
    heads = cols // HS
    phase, strip = rows // R1, rows // R2
    n_bits = n_sub.bit_length() - 1
    assert heads == 4 and n_sub == 1 << n_bits and n_seq % 2 == 0 and strip == HALF
    vmem = pl.BlockSpec(memory_space=pltpu.VMEM)
    pad = heads * FP
    return pl.pallas_call(
        functools.partial(kernel, n_seq, n_sub, heads),
        out_shape=jax.ShapeDtypeStruct((cols, rows), BF),
        in_specs=[pl.BlockSpec(memory_space=pl.ANY)] * 6,
        out_specs=vmem,
        scratch_shapes=[
            pltpu.SMEM(offsets.shape, I32),
            pltpu.SMEM(valid.shape, I32),
            pltpu.VMEM((cols, rows), BF),
            pltpu.VMEM((pad, rows), BF),
            pltpu.VMEM((pad, rows), BF),
            pltpu.VMEM(w_out.shape, BF),
            pltpu.VMEM((cols, w_out.shape[0]), BF),
            pltpu.VMEM((2, 2 * LANES, 2 * LANES), BF),
            pltpu.VMEM((R1, 4 * LANES, LANES), BF),
            pltpu.VMEM((heads, rows, FP), BF),
            pltpu.VMEM((R1, pad, phase), BF),
            pltpu.VMEM((R1, cols, phase), BF),
            pltpu.VMEM((R1, cols, phase), BF),
            pltpu.VMEM((n_seq, cols, LANES), BF),
            pltpu.VMEM((GROUP, 2, cols, phase), BF),
            pltpu.VMEM((2, rows, phase), F32),
            pltpu.VMEM((R1, cols, phase), F32),
            pltpu.VMEM((R1, 8, phase), F32),
            pltpu.VMEM((pad, phase), F32),
            pltpu.VMEM((8, phase), F32),
            pltpu.VMEM((pad, phase), F32),
            pltpu.VMEM((n_sub, R1, cols, phase), BF),
            pltpu.SemaphoreType.DMA((2, n_seq)),
            pltpu.SemaphoreType.DMA((n_seq,)),
            pltpu.SemaphoreType.DMA((2, GROUP, 2)),
            pltpu.SemaphoreType.DMA((GROUP, 2)),
            pltpu.SemaphoreType.DMA((n_bits, n_sub, R1 + 1)),
            pltpu.SemaphoreType.DMA((n_sub, R1 + 1)),
            pltpu.SemaphoreType.DMA((2 * heads + 4,)),
        ],
        compiler_params=pltpu.CompilerParams(
            collective_id=0, has_side_effects=True, vmem_limit_bytes=56 * 1024 * 1024
        ),
    )(q_heads.T, k_heads.T, v_heads.T, w_out, offsets, valid).T


def solution(mesh):
    spread = P(("slides", "seq"), "sub")
    return jax.shard_map(
        functools.partial(local, mesh.shape["seq"], mesh.shape["sub"]),
        mesh=mesh,
        in_specs=(spread, spread, spread, P(), P(), P("slides")),
        out_specs=spread,
        check_vma=False,
    )
```

```python
import functools

import jax
import jax.numpy as jnp
from jax import lax
from jax.experimental import pallas as pl
from jax.experimental.pallas import tpu as pltpu
from jax.sharding import PartitionSpec as P

HS = 48
FP = 64
GROUP = 4
R1 = 4
R2 = 16
LANES = 128
HALF = 64
MASKED = -1e30
MESH = pl.DeviceIdType.MESH
EXP_SCALE = HS ** (-0.5) * 1.4426950408889634
LOG2E = 1.4426950408889634
CONTRACT_LAST = (((1,), (1,)), ((), ()))
BF, F32, I32 = jnp.bfloat16, jnp.float32, jnp.int32


def iota(shape, dim):
    return lax.broadcasted_iota(I32, shape, dim)


def mm(a, b):
    return jnp.dot(a, b, preferred_element_type=F32)


def mm_t(a, b):
    return lax.dot_general(a, b, CONTRACT_LAST, preferred_element_type=F32)


def combine(parts):
    top = functools.reduce(jnp.maximum, [lse for _, lse in parts])
    weights = [jnp.exp2(lse - top) for _, lse in parts]
    scale = 1.0 / functools.reduce(jnp.add, weights)
    return functools.reduce(jnp.add, [o * (w * scale) for (o, _), w in zip(parts, weights)])


def kernel(
    n_seq, n_sub, heads,
    q_hbm, k_hbm, v_hbm, w_hbm, off_hbm, valid_hbm, o_ref,
    off_ref, valid_ref,
    q_ref, k_aug, v_aug, w_ref, wt, wt_last,
    perm, sel, kr, pq, pk, pv, wide, mid,
    guest, mq, mkr, mv, ret, fin_o, fin_l,
    scores, near_o, near_l, mid_o, mid_m, spread, xg, xl,
    wide_send, wide_recv, mid_send, mid_recv, q_sem, ret_send, ret_recv, x_send, x_recv, in_sem,
):
    cols, rows = q_ref.shape
    phase = rows // R1
    strip = rows // R2
    square = 2 * LANES
    seq = lax.axis_index("seq")
    sub = lax.axis_index("sub")
    pos = lax.rem(seq, GROUP)
    group0 = seq - pos
    partner = pos ^ 1
    across = GROUP - 1 - pos
    far = across ^ 1
    is_host = (pos == 1) | (pos == 2)
    is_guest = jnp.logical_not(is_host)
    bits = [1 << b for b in reversed(range(n_sub.bit_length() - 1))]

    small = [
        pltpu.make_async_copy(off_hbm, off_ref, in_sem.at[4]),
        pltpu.make_async_copy(valid_hbm, valid_ref, in_sem.at[5]),
    ]
    for copy in small:
        copy.start()
    for i, (src, dst) in enumerate(((k_hbm, k_aug), (v_hbm, v_aug))):
        for h in range(heads):
            pltpu.make_async_copy(
                src.at[pl.ds(h * HS, HS), :], dst.at[pl.ds(h * FP, HS), :], in_sem.at[i]
            ).start()
    q_fetch = pltpu.make_async_copy(q_hbm, q_ref, in_sem.at[2])
    w_fetch = pltpu.make_async_copy(w_hbm, w_ref, in_sem.at[3])
    q_fetch.start()
    barrier = pltpu.get_barrier_semaphore()
    for step, there in ((1, seq < n_seq - 1), (-1, seq > 0)):
        @pl.when(there)
        def _():
            pl.semaphore_signal(
                barrier, inc=1, device_id={"seq": seq + step}, device_id_type=MESH
            )
    for x in range(1, n_sub):
        pl.semaphore_signal(barrier, inc=1, device_id={"sub": sub ^ x}, device_id_type=MESH)

    low = iota((1, LANES), 1) < HALF
    block0 = seq * rows

    def plan(head):
        o0, o1 = off_ref[0, head], off_ref[1, head]
        m1 = lax.rem(o1, R1)
        late = o0
        second = jnp.where(m1 == o0, lax.rem(o0 + 1, R1), m1)
        third = 0
        for m in reversed(range(R1 - 1)):
            third = jnp.where((late != m) & (second != m), m, third)
        return o0, m1, lax.div(o1, R1), (late, second, third, 6 - late - second - third)

    with jax.named_scope("consts"):
        tok, at = iota((square, square), 0), iota((square, square), 1)
        for odd in range(2):
            hit = tok == at % HALF * R1 + ((at // HALF) ^ odd)
            perm[odd] = jnp.where(hit, 1.0, 0.0).astype(BF)
        at_l, at_j = iota((square, LANES), 0), iota((square, LANES), 1)
        for a in range(R1):
            for half in range(2):
                hit = at_l == (at_j - half * HALF) * R1 + a
                sel[a, pl.ds(half * square, square), :] = jnp.where(hit, 1.0, 0.0).astype(BF)
        for copy in small:
            copy.wait()
        limit = valid_ref[0]
        plans = [plan(sub * heads + h) for h in range(heads)]
        tail_one = jnp.where(iota((FP - HS, square), 0) == 0, 1.0, 0.0).astype(BF)
        for h in range(heads):
            tail = pl.ds(h * FP + HS, FP - HS)
            for m in range(R1):
                pq[m, tail, :] = tail_one
            place = block0 + iota((FP - HS, rows), 1)
            first = iota((FP - HS, rows), 0) == 0
            v_aug[tail, :] = jnp.where(first, 1.0, 0.0).astype(BF)
            k_aug[tail, :] = jnp.where(first & (place >= limit), MASKED, 0.0).astype(BF)

    def permuted(lhs_of, store):
        for c in range(rows // (2 * square)):
            outs = [
                mm(lhs_of(pl.ds((2 * c + b) * square, square)), perm[b]) for b in range(2)
            ]
            for m in range(R1):
                half = slice((m // 2) * LANES, (m // 2 + 1) * LANES)
                even, odd = outs[0][:, half], outs[1][:, half]
                if m % 2:
                    even, odd = odd, even
                store(m, slice(c * LANES, (c + 1) * LANES), jnp.where(low, even, odd).astype(BF))

    with jax.named_scope("load"):
        for i, src in enumerate((k_hbm, v_hbm)):
            pltpu.make_async_copy(src, q_ref, in_sem.at[i]).wait()
        w_fetch.start()

        def store_kv(m, lanes, val):
            pk[m, :, lanes] = val[:cols]
            pv[m, :, lanes] = val[cols:]

        permuted(
            lambda t: jnp.concatenate(
                [ref[pl.ds(h * FP, HS), t] for ref in (k_aug, v_aug) for h in range(heads)], axis=0
            ),
            store_kv,
        )
        for h in range(heads):
            o0, m1, a, _ = plans[h]
            feat = pl.ds(h * HS, HS)
            mid[pos, h, pl.ds(0, HS), :] = pk[o0, feat, :]
            mid[pos, h, pl.ds(HS, HS), :] = pv[o0, feat, :]
            both = jnp.concatenate([pk[m1, feat, :], pv[m1, feat, :]], axis=1)
            wide[seq, feat, :] = mm(both, sel[a]).astype(BF)

    with jax.named_scope("barrier"):
        inner = (seq > 0) & (seq < n_seq - 1)

        @pl.when(inner)
        def _():
            pl.semaphore_wait(barrier, n_sub - 1 + 2)

        @pl.when(jnp.logical_not(inner))
        def _():
            pl.semaphore_wait(barrier, n_sub - 1 + 1)

    def wide_copy(origin, rightward):
        target = seq + 1 if rightward else seq - 1
        return pltpu.make_async_remote_copy(
            src_ref=wide.at[origin], dst_ref=wide.at[origin],
            send_sem=wide_send.at[0], recv_sem=wide_recv.at[origin],
            device_id={"seq": target}, device_id_type=MESH,
        )

    def wide_relay(dist):
        @pl.when(seq - dist >= 0)
        def _():
            wide_copy(seq - dist, True).wait_recv()

            @pl.when(seq < n_seq - 1)
            def _():
                wide_copy(seq - dist, True).start()

        @pl.when(seq + dist < n_seq)
        def _():
            wide_copy(seq + dist, False).wait_recv()

            @pl.when(seq > 0)
            def _():
                wide_copy(seq + dist, False).start()

    def mid_copy(origin, h, kind, count=1):
        ref = mid.at[origin, h if count == 1 else pl.ds(h, count)]
        return pltpu.make_async_remote_copy(
            src_ref=ref, dst_ref=ref,
            send_sem=mid_send.at[0], recv_sem=mid_recv.at[kind, max(h - 1, 0)],
            device_id={"seq": group0 + 1 + lax.rem(pos, 2)}, device_id_type=MESH,
        )

    def mid_arrived(origin, kind, heads_of):
        if heads_of == (0, 1):
            mid_copy(origin, 0, kind, 2).wait_recv()
        else:
            for h in heads_of:
                mid_copy(origin, h, kind).wait_recv()

    own_kind = jnp.where(is_host, 1, 0)

    def q_copy():
        return pltpu.make_async_remote_copy(
            src_ref=guest, dst_ref=guest, send_sem=q_sem.at[0], recv_sem=q_sem.at[1],
            device_id={"seq": group0 + partner}, device_id_type=MESH,
        )

    def ret_copy(h, count=1):
        ref = ret.at[h if count == 1 else pl.ds(h, count)]
        return pltpu.make_async_remote_copy(
            src_ref=ref, dst_ref=ref,
            send_sem=ret_send.at[0], recv_sem=ret_recv.at[max(h - 1, 0)],
            device_id={"seq": group0 + partner}, device_id_type=MESH,
        )

    def relay(heads_of):
        mid_arrived(partner, 0, heads_of)
        for h in heads_of:
            mid_copy(partner, h, 2).start()

    @pl.when(seq < n_seq - 1)
    def _():
        wide_copy(seq, True).start()

    @pl.when(seq > 0)
    def _():
        wide_copy(seq, False).start()

    for h in range(3):
        mid_copy(pos, h, own_kind).start()

    spans = {1: (0, 2), 2: (2, 1), 3: (3, 1)}
    direct = 3
    onward = [(bit, x) for bit in bits for x in range(1, n_sub) if not x % (2 * bit)]

    def x_ref(block, group, slab=None):
        if group:
            first, count = spans[group]
            return xl.at[block, pl.ds(first * HS, count * HS)]
        return xg.at[block] if slab is None else xg.at[block, slab - 1]

    def x_copy(ref, held, bit, group):
        return pltpu.make_async_remote_copy(
            src_ref=ref, dst_ref=ref, send_sem=x_send.at[1 if group else 0],
            recv_sem=x_recv.at[(held ^ bit) - 1, group],
            device_id={"sub": sub ^ bit}, device_id_type=MESH,
        )

    def x_start(group, slab=None):
        ref = x_ref(sub, group, slab)
        for bit in (reversed(range(1, n_sub)) if group == direct else bits):
            x_copy(ref, 0, bit, group).start()

    def x_arrived(x, group):
        x_copy(x_ref(sub ^ x, group), 0, x, group).wait_recv()

    def x_forward(group):
        waited = set()
        for bit, x in onward:
            if x not in waited:
                waited.add(x)
                x_arrived(x, group)
            x_copy(x_ref(sub ^ x, group), x, bit, group).start()

    with jax.named_scope("load_q"):
        q_fetch.wait()

        def store_q(m, lanes, val):
            for h in range(heads):
                pq[m, pl.ds(h * FP, HS), lanes] = val[h * HS:(h + 1) * HS]

        permuted(lambda t: q_ref[:, t], store_q)
        for h in range(heads):
            o0 = plans[h][0]
            mq[pl.ds(h * FP, FP), pl.ds(0, phase)] = pq[o0, pl.ds(h * FP, FP), :]

        @pl.when(is_guest)
        def _():
            for h in range(heads):
                guest[pl.ds(h * HS, HS), :] = pq[plans[h][0], pl.ds(h * FP, HS), :]

    @pl.when(is_guest)
    def _():
        mid_copy(pos, 3, own_kind).start()
        q_copy().start()

    with jax.named_scope("prep"):
        for h in range(heads):
            kr[h] = k_aug[pl.ds(h * FP, FP), :].T

    def attend(keys, values, queries, before=None):
        scores = mm(keys, queries)
        peak = jnp.max(scores, axis=0, keepdims=True)
        if before is not None:
            peak = jnp.maximum(peak, before)
        probs = jnp.exp2((scores - peak) * EXP_SCALE).astype(BF)
        return peak, mm(values, probs)

    def finish(peak, out):
        mass = out[HS:HS + 1]
        return out[:HS] * (1.0 / mass), peak * EXP_SCALE + jnp.log(mass) * LOG2E

    def pipeline(jobs, pieces, keys, queries, values, done):
        def score(i, c, peak):
            part = mm(keys(jobs[i], c), queries(jobs[i]))
            scores[i % 2, pl.ds(c * phase, phase), :] = part
            top = jnp.max(part, axis=0, keepdims=True)
            return top if peak is None else jnp.maximum(peak, top)

        peak = None
        for c in range(pieces):
            peak = score(0, c, peak)
        for i, job in enumerate(jobs):
            ahead = acc = None
            for c in range(pieces):
                if i + 1 < len(jobs):
                    ahead = score(i + 1, c, ahead)
                part = scores[i % 2, pl.ds(c * phase, phase), :]
                probs = jnp.exp2((part - peak) * EXP_SCALE).astype(BF)
                out = mm(values(job, c), probs)
                acc = out if acc is None else acc + out
            done(i, job, peak, acc)
            peak = ahead

    def near_done(i, job, peak, acc):
        m, h = job
        out, lse = finish(peak, acc)
        near_o[m, pl.ds(h * HS, HS), :] = out
        near_l[m, pl.ds(h, 1), :] = lse
        for when, mine in ((6, lax.rem(sub, 2) == 1), (8, lax.rem(sub, 2) == 0)):
            if i == when:
                @pl.when(mine)
                def _():
                    wide_relay(1)

                    @pl.when(is_host)
                    def _():
                        mid_copy(pos, 3, own_kind).start()

    with jax.named_scope("near"):
        pipeline(
            [(m, h) for m in range(R1) for h in range(heads)],
            rows // phase,
            lambda job, c: kr[job[1], pl.ds(c * phase, phase), :],
            lambda job: pq[job[0], pl.ds(job[1] * FP, FP), :],
            lambda job, c: v_aug[pl.ds(job[1] * FP, FP), pl.ds(c * phase, phase)],
            near_done,
        )

    def ship(slab, h, val):
        at = pl.ds(h * HS, HS)
        if slab:
            xg[sub, slab - 1, at, :] = val.astype(BF)
        else:
            xl[sub, at, :] = val.astype(BF)

    with jax.named_scope("ship_near"):
        for slab in (2, 3):
            for h in range(heads):
                ship(slab, h, near_o[plans[h][3][slab], pl.ds(h * HS, HS), :])
            x_start(0, slab)

    ones_tail = jnp.where(iota((FP - HS, phase), 0) == 0, 1.0, 0.0).astype(BF)

    def split(lse, width):
        top = jnp.floor(lse * 0.25) * 4.0
        rest = lse - top
        middle = jnp.floor(rest * 64.0) * (1.0 / 64.0)
        r = iota((FP - HS, width), 0)
        low_part = jnp.where(r == 2, rest - middle, jnp.where(r == 3, 1.0, 0.0))
        return jnp.where(r == 0, top, jnp.where(r == 1, middle, low_part))

    def joined(rows_of):
        return rows_of[0:1] + rows_of[1:2] + rows_of[2:3]

    def mid_kv(origin, h):
        o0 = plans[h][0]
        lane = iota((FP - HS, phase), 1)
        at = jnp.where(lax.rem(o0, 2) == 1, lane ^ HALF, lane)
        place = (group0 + origin) * rows + at * R1 + o0
        dead = (iota((FP - HS, phase), 0) == 0) & (place >= limit)
        dead = jnp.where(dead, MASKED, 0.0).astype(BF)
        return (
            jnp.concatenate([mid[origin, h, pl.ds(0, HS), :], dead], axis=0).T,
            jnp.concatenate([mid[origin, h, pl.ds(HS, HS), :], ones_tail], axis=0),
        )

    def mid_stage(origin, slot):
        for h in range(heads):
            at = pl.ds(slot * phase, phase)
            mkr[h, at, :], mv[pl.ds(h * FP, FP), at] = mid_kv(origin, h)

    def mid_pass():
        def done(i, job, peak, acc):
            h, t = job
            at = pl.ds(t * phase, phase)
            mid_m[pl.ds(h, 1), at] = peak
            mid_o[pl.ds(h * FP, FP), at] = acc

        pipeline(
            [(h, t) for h in range(heads) for t in range(2)],
            GROUP - 1,
            lambda job, c: mkr[job[0], pl.ds(c * phase, phase), :],
            lambda job: mq[pl.ds(job[0] * FP, FP), pl.ds(job[1] * phase, phase)],
            lambda job, c: mv[pl.ds(job[0] * FP, FP), pl.ds(c * phase, phase)],
            done,
        )

    def mid_step(origin, heads_of):
        staged = [mid_kv(origin, h) for h in heads_of]
        scored = [
            mm(keys, mq[pl.ds(h * FP, FP), :]) for h, (keys, _) in zip(heads_of, staged)
        ]
        fore = [(mid_m[pl.ds(h, 1), :], mid_o[pl.ds(h * FP, FP), :]) for h in heads_of]
        done = []
        for score, (_, vals), (before, _) in zip(scored, staged, fore):
            peak = jnp.maximum(jnp.max(score, axis=0, keepdims=True), before)
            probs = jnp.exp2((score - peak) * EXP_SCALE).astype(BF)
            done.append((peak, mm(vals, probs)))
        return [
            (peak, out + old * jnp.exp2((before - peak) * EXP_SCALE))
            for (peak, out), (before, old) in zip(done, fore)
        ]

    def hosted(name, steps):
        @pl.when(is_host)
        def _():
            with jax.named_scope(name):
                for step in steps:
                    step()

    def guest_queries():
        q_copy().wait_recv()
        for h in range(heads):
            at = pl.ds(phase, phase)
            mq[pl.ds(h * FP, HS), at] = guest[pl.ds(h * HS, HS), :]
            mq[pl.ds(h * FP + HS, FP - HS), at] = tail_one

    early, later = (0, 1), (2, 3)
    hosted("relay", [lambda: relay(early), lambda: relay(later)])
    with jax.named_scope("wide_relay2"):
        wide_relay(2)
    hosted("mid_stage", [
        lambda: mid_stage(pos, 0),
        lambda: mid_stage(partner, 1),
        lambda: mid_arrived(across, 1, early),
        lambda: mid_arrived(across, 1, later),
        lambda: mid_stage(across, 2),
    ])
    hosted("guest_q", [guest_queries])
    hosted("mid_pass", [mid_pass])
    def mid_last(heads_of):
        mid_arrived(far, 2, heads_of)
        done = mid_step(far, heads_of)
        for h, (peak, out) in zip(heads_of, done):
            o, lse = finish(peak, out)
            feat = pl.ds(h * FP, HS)
            ret[h, pl.ds(0, HS), :] = o[:, phase:].astype(BF)
            ret[h, pl.ds(HS, FP - HS), :] = split(lse[:, phase:], phase).astype(BF)
            ret_copy(h).start()
            fin_o[pl.ds(h * HS, HS), :] = o[:, :phase]
            fin_l[pl.ds(h, 1), :] = lse[:, :phase]

    hosted("mid_last01", [lambda: mid_last(early)])
    hosted("mid_last2", [lambda: mid_last((2,))])
    hosted("mid_last3", [lambda: mid_last((3,))])
    with jax.named_scope("weights"):
        w_fetch.wait()
        for s in range(n_sub):
            @pl.when(sub == s)
            def _():
                mine = slice(s * cols, (s + 1) * cols)
                wt[...] = w_ref[:, mine].T
                wt_last[...] = jnp.concatenate(
                    [w_ref[(d + 1) * cols - HS:(d + 1) * cols, mine] for d in range(n_sub)], axis=0
                ).T
    with jax.named_scope("wide_relay3"):
        for dist in range(3, n_seq):
            wide_relay(dist)

    with jax.named_scope("wide"):
        q_rows = []
        for h in range(heads):
            _, m1, a, _ = plans[h]
            q_h = mm(pq[m1, pl.ds(h * FP, FP), :], sel[a, pl.ds((h % 2) * square, square), :])
            zero = jnp.zeros((FP, LANES), BF)
            q_h = q_h.astype(BF)
            q_rows.append(jnp.concatenate([q_h, zero] if h < 2 else [zero, q_h], axis=1))
        q_wide = jnp.concatenate(q_rows, axis=0)
        keys, values = [], []
        zeros_tail = jnp.zeros((FP - HS - 8, LANES), F32)
        for pr in range(n_seq // 2):
            one, two = [wide[2 * pr + i].astype(F32) for i in range(2)]
            k_pair = jnp.where(low, one, pltpu.roll(two, HALF, 1))
            v_pair = jnp.where(low, pltpu.roll(one, HALF, 1), two)
            k_rows, v_rows = [], []
            for h in range(heads):
                _, m1, a, _ = plans[h]
                lane = iota((FP - HS, LANES), 1)
                row0 = iota((FP - HS, LANES), 0) == 0
                at = lane % HALF * R1 + a
                at = jnp.where(lax.rem(m1, 2) == 1, at ^ HALF, at)
                place = (2 * pr + lane // HALF) * rows + at * R1 + m1
                k_rows += [
                    k_pair[h * HS:(h + 1) * HS],
                    jnp.where(row0 & (place >= limit), MASKED, 0.0),
                ]
                v_rows += [v_pair[h * HS:(h + 1) * HS], jnp.where(row0, 1.0, 0.0)]
            keys.append(jnp.concatenate(k_rows, axis=0).astype(BF).T)
            values.append(jnp.concatenate(v_rows, axis=0).astype(BF))
        peak, out = attend(
            jnp.concatenate(keys, axis=0), jnp.concatenate(values, axis=1), q_wide
        )
        for h in range(heads):
            _, m1, a, _ = plans[h]
            col = slice((h // 2) * LANES, (h // 2 + 1) * LANES)
            o_h, lse = finish(peak[:, col], out[h * FP:(h + 1) * FP, col])
            z = jnp.concatenate([o_h, split(lse, LANES)], axis=0).astype(BF)
            put = mm_t(z, sel[a, pl.ds((h % 2) * square, square), :])
            spread[pl.ds(h * FP, HS), :] = put[:HS]
            lse = joined(put[HS:])
            lse = jnp.where(put[HS + 3:HS + 4] > 0.5, lse, MASKED)
            spread[pl.ds(h * FP + HS, 8), :] = jnp.broadcast_to(lse, (8, phase))
            two = plans[h][3][1]
            feat = pl.ds(h * HS, HS)
            lse = jnp.where(two == m1, lse, MASKED)
            ship(1, h, combine([
                (near_o[two, feat, :], near_l[two, pl.ds(h, 1), :]), (put[:HS], lse),
            ]))
        x_start(0, 1)

    def returned(heads_of):
        if heads_of == (0, 1):
            ret_copy(0, 2).wait_recv()
        else:
            ret_copy(heads_of[0]).wait_recv()
        for h in heads_of:
            fin_o[pl.ds(h * HS, HS), :] = ret[h, pl.ds(0, HS), :].astype(F32)
            fin_l[pl.ds(h, 1), :] = joined(ret[h, pl.ds(HS, FP - HS), :].astype(F32))

    def conclude(heads_of):
        for h in heads_of:
            o0, m1 = plans[h][:2]
            feat = pl.ds(h * HS, HS)
            lse_w = spread[pl.ds(h * FP + HS, 1), :]
            ship(0, h, combine([
                (near_o[o0, feat, :], near_l[o0, pl.ds(h, 1), :]),
                (fin_o[feat, :], fin_l[pl.ds(h, 1), :]),
                (spread[pl.ds(h * FP, HS), :], jnp.where(m1 == o0, lse_w, MASKED)),
            ]))

    def guested(name, steps):
        @pl.when(is_guest)
        def _():
            with jax.named_scope(name):
                for step in steps:
                    step()

    guested("back01", [lambda: returned(early)])
    with jax.named_scope("conclude01"):
        conclude(early)
        x_start(1)
    for h in later:
        guested(f"back{h}", [lambda: returned((h,))])
        with jax.named_scope(f"conclude{h}"):
            conclude((h,))
            x_start(h)
    with jax.named_scope("x_fwd"):
        x_forward(0)

    with jax.named_scope("x_wait"):
        passed = {x for _, x in onward}
        for group in range(direct):
            if group:
                x_forward(group)
            for x in range(1, n_sub):
                if x not in passed:
                    x_arrived(x, group)

    every = [plan(i)[3] for i in range(n_sub * heads)]
    zeros_head = jnp.zeros((HS, phase), BF)
    with jax.named_scope("project_most"):
        for m in range(R1):
            parts = []
            for d in range(n_sub):
                for h in range(heads):
                    order = every[d * heads + h]
                    at = jnp.where(order[1] == m, 0, jnp.where(order[2] == m, 1, 2))
                    feat = pl.ds(h * HS, HS)
                    held = xl[d, feat, :] if h < heads - 1 else zeros_head
                    parts.append(jnp.where(order[0] == m, held, xg[d, at, feat, :]))
            near_o[m] = mm(wt[...], jnp.concatenate(parts, axis=0))
    with jax.named_scope("x_last"):
        for x in range(1, n_sub):
            x_arrived(x, direct)

    with jax.named_scope("project"):
        outs = []
        for m in range(R1):
            last = jnp.concatenate([
                jnp.where(
                    every[d * heads + heads - 1][0] == m, xl[d, pl.ds(cols - HS, HS), :], zeros_head
                )
                for d in range(n_sub)
            ], axis=0)
            outs.append((near_o[m] + mm(wt_last[...], last)).astype(BF).astype(F32))
        for c in range(rows // (2 * square)):
            at = slice(c * LANES, (c + 1) * LANES)
            for odd in range(2):
                pieces = [
                    jnp.where(low, outs[2 * i + odd][:, at], outs[2 * i + 1 - odd][:, at])
                    for i in range(2)
                ]
                res = mm_t(jnp.concatenate(pieces, axis=1).astype(BF), perm[odd])
                first = (2 * c + odd) * square
                place = block0 + first + iota((1, square), 1)
                o_ref[:, first:first + square] = jnp.where(place < limit, res, 0.0).astype(BF)

    with jax.named_scope("drain"):
        def sent(ref, sem):
            pltpu.make_async_remote_copy(
                src_ref=ref, dst_ref=ref, send_sem=sem, recv_sem=sem,
                device_id={"sub": sub ^ 1}, device_id_type=MESH,
            ).wait_send()

        @pl.when(inner)
        def _():
            sent(wide, wide_send.at[0])

        @pl.when(jnp.logical_not(inner))
        def _():
            sent(wide.at[0], wide_send.at[0])

        @pl.when(is_host)
        def _():
            sent(mid.at[pl.ds(0, 2)], mid_send.at[0])
            sent(ret, ret_send.at[0])

        @pl.when(is_guest)
        def _():
            sent(mid.at[0], mid_send.at[0])
            q_copy().wait_send()

        sent(xg.at[pl.ds(0, n_sub - 1)], x_send.at[0])
        sent(xl.at[pl.ds(0, n_sub - 1)], x_send.at[1])


def local(n_seq, n_sub, q_heads, k_heads, v_heads, w_out, offsets, valid):
    rows, cols = q_heads.shape
    heads = cols // HS
    phase, strip = rows // R1, rows // R2
    assert heads == 4 and n_sub & (n_sub - 1) == 0 and n_seq % 2 == 0 and strip == HALF
    vmem = pl.BlockSpec(memory_space=pltpu.VMEM)
    pad = heads * FP
    return pl.pallas_call(
        functools.partial(kernel, n_seq, n_sub, heads),
        out_shape=jax.ShapeDtypeStruct((cols, rows), BF),
        in_specs=[pl.BlockSpec(memory_space=pl.ANY)] * 6,
        out_specs=vmem,
        scratch_shapes=[
            pltpu.SMEM(offsets.shape, I32),
            pltpu.SMEM(valid.shape, I32),
            pltpu.VMEM((cols, rows), BF),
            pltpu.VMEM((pad, rows), BF),
            pltpu.VMEM((pad, rows), BF),
            pltpu.VMEM(w_out.shape, BF),
            pltpu.VMEM((cols, w_out.shape[0]), BF),
            pltpu.VMEM((cols, n_sub * HS), BF),
            pltpu.VMEM((2, 2 * LANES, 2 * LANES), BF),
            pltpu.VMEM((R1, 4 * LANES, LANES), BF),
            pltpu.VMEM((heads, rows, FP), BF),
            pltpu.VMEM((R1, pad, phase), BF),
            pltpu.VMEM((R1, cols, phase), BF),
            pltpu.VMEM((R1, cols, phase), BF),
            pltpu.VMEM((n_seq + 1, cols, LANES), BF),
            pltpu.VMEM((GROUP, heads, 2 * HS, phase), BF),
            pltpu.VMEM((cols, phase), BF),
            pltpu.VMEM((pad, 2 * phase), BF),
            pltpu.VMEM((heads, (GROUP - 1) * phase, FP), BF),
            pltpu.VMEM((pad, (GROUP - 1) * phase), BF),
            pltpu.VMEM((heads, FP, phase), BF),
            pltpu.VMEM((cols, phase), F32),
            pltpu.VMEM((8, phase), F32),
            pltpu.VMEM((2, rows, phase), F32),
            pltpu.VMEM((R1, cols, phase), F32),
            pltpu.VMEM((R1, 8, phase), F32),
            pltpu.VMEM((pad, 2 * phase), F32),
            pltpu.VMEM((8, 2 * phase), F32),
            pltpu.VMEM((pad, phase), F32),
            pltpu.VMEM((n_sub, R1 - 1, cols, phase), BF),
            pltpu.VMEM((n_sub, cols, phase), BF),
            pltpu.SemaphoreType.DMA((1,)),
            pltpu.SemaphoreType.DMA((n_seq,)),
            pltpu.SemaphoreType.DMA((1,)),
            pltpu.SemaphoreType.DMA((3, 3)),
            pltpu.SemaphoreType.DMA((2,)),
            pltpu.SemaphoreType.DMA((1,)),
            pltpu.SemaphoreType.DMA((3,)),
            pltpu.SemaphoreType.DMA((2,)),
            pltpu.SemaphoreType.DMA((n_sub - 1, 4)),
            pltpu.SemaphoreType.DMA((6,)),
        ],
        compiler_params=pltpu.CompilerParams(
            collective_id=0, has_side_effects=True, vmem_limit_bytes=54784 * 1024
        ),
    )(q_heads.T, k_heads.T, v_heads.T, w_out, offsets, valid).T


def solution(mesh):
    spread = P(("slides", "seq"), "sub")
    return jax.shard_map(
        functools.partial(local, mesh.shape["seq"], mesh.shape["sub"]),
        mesh=mesh,
        in_specs=(spread, spread, spread, P(), P(), P("slides")),
        out_specs=spread,
        check_vma=False,
    )
```

```python
import functools

import jax
import jax.numpy as jnp
from jax import lax
from jax.experimental import pallas as pl
from jax.experimental.pallas import tpu as pltpu
from jax.sharding import PartitionSpec as P

HS = 48
FP = 64
TAIL = 8
GROUP = 4
R1 = 4
R2 = 16
LANES = 128
HALF = 64
MASKED = -1e30
MESH = pl.DeviceIdType.MESH
EXP_SCALE = HS ** (-0.5) * 1.4426950408889634
LOG2E = 1.4426950408889634
CONTRACT_LAST = (((1,), (1,)), ((), ()))
BF, F32, I32 = jnp.bfloat16, jnp.float32, jnp.int32


def iota(shape, dim):
    return lax.broadcasted_iota(I32, shape, dim)


def mm(a, b):
    return jnp.dot(a, b, preferred_element_type=F32)


def mm_t(a, b):
    return lax.dot_general(a, b, CONTRACT_LAST, preferred_element_type=F32)


def combine(parts):
    top = functools.reduce(jnp.maximum, [lse for _, lse in parts])
    weights = [jnp.exp2(lse - top) for _, lse in parts]
    scale = 1.0 / functools.reduce(jnp.add, weights)
    return functools.reduce(jnp.add, [o * (w * scale) for (o, _), w in zip(parts, weights)])


def kernel(
    n_seq, n_sub, heads,
    q_hbm, k_hbm, v_hbm, w_hbm, off_hbm, valid_hbm, o_ref,
    off_ref, valid_ref,
    q_ref, k_aug, v_aug, w_ref, wt, wt_last,
    perm, sel, kr, pq, pk, pv, wide, mid,
    guest, mq, mkr, mv, ret, fin_o, fin_l,
    scores, near_o, near_l, mid_o, mid_m, spread, xg, xl,
    wide_send, wide_recv, mid_send, mid_recv, q_sem, ret_send, ret_recv, x_send, x_recv, in_sem,
):
    cols, rows = q_ref.shape
    phase = rows // R1
    strip = rows // R2
    square = 2 * LANES
    seq = lax.axis_index("seq")
    sub = lax.axis_index("sub")
    pos = lax.rem(seq, GROUP)
    group0 = seq - pos
    partner = pos ^ 1
    across = GROUP - 1 - pos
    far = across ^ 1
    is_host = (pos == 1) | (pos == 2)
    is_guest = jnp.logical_not(is_host)
    bits = [1 << b for b in reversed(range(n_sub.bit_length() - 1))]

    small = [
        pltpu.make_async_copy(off_hbm, off_ref, in_sem.at[4]),
        pltpu.make_async_copy(valid_hbm, valid_ref, in_sem.at[5]),
    ]
    for copy in small:
        copy.start()
    for i, (src, dst) in enumerate(((k_hbm, k_aug), (v_hbm, v_aug))):
        for h in range(heads):
            pltpu.make_async_copy(
                src.at[pl.ds(h * HS, HS), :], dst.at[pl.ds(h * FP, HS), :], in_sem.at[i]
            ).start()
    q_fetch = pltpu.make_async_copy(q_hbm, q_ref, in_sem.at[2])
    w_fetch = pltpu.make_async_copy(w_hbm, w_ref, in_sem.at[3])
    q_fetch.start()
    barrier = pltpu.get_barrier_semaphore()
    for step, there in ((1, seq < n_seq - 1), (-1, seq > 0)):
        @pl.when(there)
        def _():
            pl.semaphore_signal(
                barrier, inc=1, device_id={"seq": seq + step}, device_id_type=MESH
            )
    for x in range(1, n_sub):
        pl.semaphore_signal(barrier, inc=1, device_id={"sub": sub ^ x}, device_id_type=MESH)

    low = iota((1, LANES), 1) < HALF
    block0 = seq * rows

    def plan(head):
        o0, o1 = off_ref[0, head], off_ref[1, head]
        m1 = lax.rem(o1, R1)
        late = o0
        second = jnp.where(m1 == o0, lax.rem(o0 + 1, R1), m1)
        third = 0
        for m in reversed(range(R1 - 1)):
            third = jnp.where((late != m) & (second != m), m, third)
        return o0, m1, lax.div(o1, R1), (late, second, third, 6 - late - second - third)

    with jax.named_scope("consts"):
        tok, at = iota((square, square), 0), iota((square, square), 1)
        for odd in range(2):
            hit = tok == at % HALF * R1 + ((at // HALF) ^ odd)
            perm[odd] = jnp.where(hit, 1.0, 0.0).astype(BF)
        at_l, at_j = iota((square, LANES), 0), iota((square, LANES), 1)
        for a in range(R1):
            for half in range(2):
                hit = at_l == (at_j - half * HALF) * R1 + a
                sel[a, pl.ds(half * square, square), :] = jnp.where(hit, 1.0, 0.0).astype(BF)
        for copy in small:
            copy.wait()
        limit = valid_ref[0]
        plans = [plan(sub * heads + h) for h in range(heads)]
        tail_one = jnp.where(iota((FP - HS, square), 0) == 0, 1.0, 0.0).astype(BF)
        for h in range(heads):
            tail = pl.ds(h * FP + HS, FP - HS)
            for m in range(R1):
                pq[m, tail, :] = tail_one
            place = block0 + iota((FP - HS, rows), 1)
            first = iota((FP - HS, rows), 0) == 0
            v_aug[tail, :] = jnp.where(first, 1.0, 0.0).astype(BF)
            k_aug[tail, :] = jnp.where(first & (place >= limit), MASKED, 0.0).astype(BF)

    def permuted(lhs_of, store):
        for c in range(rows // (2 * square)):
            outs = [
                mm(lhs_of(pl.ds((2 * c + b) * square, square)), perm[b]) for b in range(2)
            ]
            for m in range(R1):
                half = slice((m // 2) * LANES, (m // 2 + 1) * LANES)
                even, odd = outs[0][:, half], outs[1][:, half]
                if m % 2:
                    even, odd = odd, even
                store(m, slice(c * LANES, (c + 1) * LANES), jnp.where(low, even, odd).astype(BF))

    with jax.named_scope("load"):
        for i, src in enumerate((k_hbm, v_hbm)):
            pltpu.make_async_copy(src, q_ref, in_sem.at[i]).wait()
        w_fetch.start()

        def store_kv(m, lanes, val):
            pk[m, :, lanes] = val[:cols]
            pv[m, :, lanes] = val[cols:]

        permuted(
            lambda t: jnp.concatenate(
                [ref[pl.ds(h * FP, HS), t] for ref in (k_aug, v_aug) for h in range(heads)], axis=0
            ),
            store_kv,
        )
        for h in range(heads):
            o0, m1, a, _ = plans[h]
            feat = pl.ds(h * HS, HS)
            mid[pos, h, pl.ds(0, HS), :] = pk[o0, feat, :]
            mid[pos, h, pl.ds(HS, HS), :] = pv[o0, feat, :]
            both = jnp.concatenate([pk[m1, feat, :], pv[m1, feat, :]], axis=1)
            wide[seq, feat, :] = mm(both, sel[a]).astype(BF)

    with jax.named_scope("barrier"):
        inner = (seq > 0) & (seq < n_seq - 1)

        @pl.when(inner)
        def _():
            pl.semaphore_wait(barrier, n_sub - 1 + 2)

        @pl.when(jnp.logical_not(inner))
        def _():
            pl.semaphore_wait(barrier, n_sub - 1 + 1)

    def wide_copy(origin, rightward):
        target = seq + 1 if rightward else seq - 1
        return pltpu.make_async_remote_copy(
            src_ref=wide.at[origin], dst_ref=wide.at[origin],
            send_sem=wide_send.at[0], recv_sem=wide_recv.at[origin],
            device_id={"seq": target}, device_id_type=MESH,
        )

    def wide_relay(dist):
        @pl.when(seq - dist >= 0)
        def _():
            wide_copy(seq - dist, True).wait_recv()

            @pl.when(seq < n_seq - 1)
            def _():
                wide_copy(seq - dist, True).start()

        @pl.when(seq + dist < n_seq)
        def _():
            wide_copy(seq + dist, False).wait_recv()

            @pl.when(seq > 0)
            def _():
                wide_copy(seq + dist, False).start()

    def mid_copy(origin, h, kind, count=1):
        ref = mid.at[origin, h if count == 1 else pl.ds(h, count)]
        return pltpu.make_async_remote_copy(
            src_ref=ref, dst_ref=ref,
            send_sem=mid_send.at[0], recv_sem=mid_recv.at[kind, max(h - 1, 0)],
            device_id={"seq": group0 + 1 + lax.rem(pos, 2)}, device_id_type=MESH,
        )

    def mid_arrived(origin, kind, heads_of):
        if heads_of == (0, 1):
            mid_copy(origin, 0, kind, 2).wait_recv()
        else:
            for h in heads_of:
                mid_copy(origin, h, kind).wait_recv()

    own_kind = jnp.where(is_host, 1, 0)

    def q_copy():
        return pltpu.make_async_remote_copy(
            src_ref=guest, dst_ref=guest, send_sem=q_sem.at[0], recv_sem=q_sem.at[1],
            device_id={"seq": group0 + partner}, device_id_type=MESH,
        )

    def ret_copy(h, count=1):
        ref = ret.at[h if count == 1 else pl.ds(h, count)]
        return pltpu.make_async_remote_copy(
            src_ref=ref, dst_ref=ref,
            send_sem=ret_send.at[0], recv_sem=ret_recv.at[max(h - 1, 0)],
            device_id={"seq": group0 + partner}, device_id_type=MESH,
        )

    def relay(heads_of):
        mid_arrived(partner, 0, heads_of)
        for h in heads_of:
            mid_copy(partner, h, 2).start()

    @pl.when(seq < n_seq - 1)
    def _():
        wide_copy(seq, True).start()

    @pl.when(seq > 0)
    def _():
        wide_copy(seq, False).start()

    for h in range(3):
        mid_copy(pos, h, own_kind).start()

    spans = {1: (0, 2), 2: (2, 1), 3: (3, 1)}
    direct = 3
    onward = [(bit, x) for bit in bits for x in range(1, n_sub) if not x % (2 * bit)]

    def x_ref(block, group, slab=None):
        if group:
            first, count = spans[group]
            return xl.at[block, pl.ds(first * HS, count * HS)]
        return xg.at[block] if slab is None else xg.at[block, slab - 1]

    def x_copy(ref, held, bit, group):
        return pltpu.make_async_remote_copy(
            src_ref=ref, dst_ref=ref, send_sem=x_send.at[1 if group else 0],
            recv_sem=x_recv.at[(held ^ bit) - 1, group],
            device_id={"sub": sub ^ bit}, device_id_type=MESH,
        )

    def x_start(group, slab=None):
        ref = x_ref(sub, group, slab)
        for bit in (reversed(range(1, n_sub)) if group == direct else bits):
            x_copy(ref, 0, bit, group).start()

    def x_arrived(x, group):
        x_copy(x_ref(sub ^ x, group), 0, x, group).wait_recv()

    def x_forward(group):
        waited = set()
        for bit, x in onward:
            if x not in waited:
                waited.add(x)
                x_arrived(x, group)
            x_copy(x_ref(sub ^ x, group), x, bit, group).start()

    with jax.named_scope("load_q"):
        q_fetch.wait()

        def store_q(m, lanes, val):
            for h in range(heads):
                pq[m, pl.ds(h * FP, HS), lanes] = val[h * HS:(h + 1) * HS]

        permuted(lambda t: q_ref[:, t], store_q)
        for h in range(heads):
            o0 = plans[h][0]
            mq[pl.ds(h * FP, FP), pl.ds(0, phase)] = pq[o0, pl.ds(h * FP, FP), :]

        @pl.when(is_guest)
        def _():
            for h in range(heads):
                guest[pl.ds(h * HS, HS), :] = pq[plans[h][0], pl.ds(h * FP, HS), :]

    @pl.when(is_guest)
    def _():
        mid_copy(pos, 3, own_kind).start()
        q_copy().start()

    with jax.named_scope("prep"):
        for h in range(heads):
            kr[h] = k_aug[pl.ds(h * FP, FP), :].T

    def attend(keys, values, queries, before=None):
        scores = mm(keys, queries)
        peak = jnp.max(scores, axis=0, keepdims=True)
        if before is not None:
            peak = jnp.maximum(peak, before)
        probs = jnp.exp2((scores - peak) * EXP_SCALE).astype(BF)
        return peak, mm(values, probs)

    def finish(peak, out):
        mass = out[HS:HS + 1]
        return out[:HS] * (1.0 / mass), peak * EXP_SCALE + jnp.log(mass) * LOG2E

    def pipeline(jobs, pieces, keys, queries, values, done):
        def score(i, c, peak):
            part = mm(keys(jobs[i], c), queries(jobs[i]))
            scores[i % 2, pl.ds(c * phase, phase), :] = part
            top = jnp.max(part, axis=0, keepdims=True)
            return top if peak is None else jnp.maximum(peak, top)

        peak = None
        for c in range(pieces):
            peak = score(0, c, peak)
        for i, job in enumerate(jobs):
            ahead = acc = None
            for c in range(pieces):
                if i + 1 < len(jobs):
                    ahead = score(i + 1, c, ahead)
                part = scores[i % 2, pl.ds(c * phase, phase), :]
                probs = jnp.exp2((part - peak) * EXP_SCALE).astype(BF)
                out = mm(values(job, c), probs)
                acc = out if acc is None else acc + out
            done(i, job, peak, acc)
            peak = ahead

    def near_done(i, job, peak, acc):
        m, h = job
        out, lse = finish(peak, acc)
        near_o[m, pl.ds(h * HS, HS), :] = out
        near_l[m, pl.ds(h, 1), :] = lse
        for when, mine in ((6, lax.rem(sub, 2) == 1), (8, lax.rem(sub, 2) == 0)):
            if i == when:
                @pl.when(mine)
                def _():
                    wide_relay(1)

                    @pl.when(is_host)
                    def _():
                        mid_copy(pos, 3, own_kind).start()

    with jax.named_scope("near"):
        pipeline(
            [(m, h) for m in range(R1) for h in range(heads)],
            rows // phase,
            lambda job, c: kr[job[1], pl.ds(c * phase, phase), :],
            lambda job: pq[job[0], pl.ds(job[1] * FP, FP), :],
            lambda job, c: v_aug[pl.ds(job[1] * FP, FP), pl.ds(c * phase, phase)],
            near_done,
        )

    def ship(slab, h, val):
        at = pl.ds(h * HS, HS)
        if slab:
            xg[sub, slab - 1, at, :] = val.astype(BF)
        else:
            xl[sub, at, :] = val.astype(BF)

    with jax.named_scope("ship_near"):
        for slab in (2, 3):
            for h in range(heads):
                ship(slab, h, near_o[plans[h][3][slab], pl.ds(h * HS, HS), :])
            x_start(0, slab)

    ones_tail = jnp.where(iota((FP - HS, phase), 0) == 0, 1.0, 0.0).astype(BF)

    def split(lse, width, count=FP - HS):
        top = jnp.floor(lse * 0.25) * 4.0
        rest = lse - top
        middle = jnp.floor(rest * 64.0) * (1.0 / 64.0)
        r = iota((count, width), 0)
        low_part = jnp.where(r == 2, rest - middle, jnp.where(r == 3, 1.0, 0.0))
        return jnp.where(r == 0, top, jnp.where(r == 1, middle, low_part))

    def joined(rows_of):
        return rows_of[0:1] + rows_of[1:2] + rows_of[2:3]

    def mid_kv(origin, h):
        o0 = plans[h][0]
        lane = iota((FP - HS, phase), 1)
        at = jnp.where(lax.rem(o0, 2) == 1, lane ^ HALF, lane)
        place = (group0 + origin) * rows + at * R1 + o0
        dead = (iota((FP - HS, phase), 0) == 0) & (place >= limit)
        dead = jnp.where(dead, MASKED, 0.0).astype(BF)
        return (
            jnp.concatenate([mid[origin, h, pl.ds(0, HS), :], dead], axis=0).T,
            jnp.concatenate([mid[origin, h, pl.ds(HS, HS), :], ones_tail], axis=0),
        )

    def mid_stage(origin, slot):
        for h in range(heads):
            at = pl.ds(slot * phase, phase)
            mkr[h, at, :], mv[pl.ds(h * FP, FP), at] = mid_kv(origin, h)

    def mid_pass():
        def done(i, job, peak, acc):
            h, t = job
            at = pl.ds(t * phase, phase)
            mid_m[pl.ds(h, 1), at] = peak
            mid_o[pl.ds(h * FP, FP), at] = acc

        pipeline(
            [(h, t) for h in range(heads) for t in range(2)],
            GROUP - 1,
            lambda job, c: mkr[job[0], pl.ds(c * phase, phase), :],
            lambda job: mq[pl.ds(job[0] * FP, FP), pl.ds(job[1] * phase, phase)],
            lambda job, c: mv[pl.ds(job[0] * FP, FP), pl.ds(c * phase, phase)],
            done,
        )

    def mid_step(origin, heads_of):
        staged = [mid_kv(origin, h) for h in heads_of]
        scored = [
            mm(keys, mq[pl.ds(h * FP, FP), :]) for h, (keys, _) in zip(heads_of, staged)
        ]
        fore = [(mid_m[pl.ds(h, 1), :], mid_o[pl.ds(h * FP, FP), :]) for h in heads_of]
        done = []
        for score, (_, vals), (before, _) in zip(scored, staged, fore):
            peak = jnp.maximum(jnp.max(score, axis=0, keepdims=True), before)
            probs = jnp.exp2((score - peak) * EXP_SCALE).astype(BF)
            done.append((peak, mm(vals, probs)))
        return [
            (peak, out + old * jnp.exp2((before - peak) * EXP_SCALE))
            for (peak, out), (before, old) in zip(done, fore)
        ]

    def hosted(name, steps):
        @pl.when(is_host)
        def _():
            with jax.named_scope(name):
                for step in steps:
                    step()

    def guest_queries():
        q_copy().wait_recv()
        for h in range(heads):
            at = pl.ds(phase, phase)
            mq[pl.ds(h * FP, HS), at] = guest[pl.ds(h * HS, HS), :]
            mq[pl.ds(h * FP + HS, FP - HS), at] = tail_one

    early, later = (0, 1), (2, 3)
    hosted("relay", [lambda: relay(early), lambda: relay(later)])
    with jax.named_scope("wide_relay2"):
        wide_relay(2)
    hosted("mid_stage", [
        lambda: mid_stage(pos, 0),
        lambda: mid_stage(partner, 1),
        lambda: mid_arrived(across, 1, early),
        lambda: mid_arrived(across, 1, later),
        lambda: mid_stage(across, 2),
    ])
    hosted("guest_q", [guest_queries])
    hosted("mid_pass", [mid_pass])
    def mid_last(heads_of):
        mid_arrived(far, 2, heads_of)
        done = mid_step(far, heads_of)
        for h, (peak, out) in zip(heads_of, done):
            o, lse = finish(peak, out)
            feat = pl.ds(h * FP, HS)
            ret[h, pl.ds(0, HS), :] = o[:, phase:].astype(BF)
            ret[h, pl.ds(HS, TAIL), :] = split(lse[:, phase:], phase, TAIL).astype(BF)
            ret_copy(h).start()
            fin_o[pl.ds(h * HS, HS), :] = o[:, :phase]
            fin_l[pl.ds(h, 1), :] = lse[:, :phase]

    hosted("mid_last01", [lambda: mid_last(early)])
    hosted("mid_last2", [lambda: mid_last((2,))])
    hosted("mid_last3", [lambda: mid_last((3,))])
    with jax.named_scope("weights"):
        w_fetch.wait()
        for s in range(n_sub):
            @pl.when(sub == s)
            def _():
                mine = slice(s * cols, (s + 1) * cols)
                wt[...] = w_ref[:, mine].T
                wt_last[...] = jnp.concatenate([
                    w_ref[d * cols + cols // 2:(d + 1) * cols, mine] for d in range(n_sub)
                ], axis=0).T
    with jax.named_scope("wide_relay3"):
        for dist in range(3, n_seq):
            wide_relay(dist)

    with jax.named_scope("wide"):
        q_rows = []
        for h in range(heads):
            _, m1, a, _ = plans[h]
            q_h = mm(pq[m1, pl.ds(h * FP, FP), :], sel[a, pl.ds((h % 2) * square, square), :])
            zero = jnp.zeros((FP, LANES), BF)
            q_h = q_h.astype(BF)
            q_rows.append(jnp.concatenate([q_h, zero] if h < 2 else [zero, q_h], axis=1))
        q_wide = jnp.concatenate(q_rows, axis=0)
        keys, values = [], []
        zeros_tail = jnp.zeros((FP - HS - 8, LANES), F32)
        for pr in range(n_seq // 2):
            one, two = [wide[2 * pr + i].astype(F32) for i in range(2)]
            k_pair = jnp.where(low, one, pltpu.roll(two, HALF, 1))
            v_pair = jnp.where(low, pltpu.roll(one, HALF, 1), two)
            k_rows, v_rows = [], []
            for h in range(heads):
                _, m1, a, _ = plans[h]
                lane = iota((FP - HS, LANES), 1)
                row0 = iota((FP - HS, LANES), 0) == 0
                at = lane % HALF * R1 + a
                at = jnp.where(lax.rem(m1, 2) == 1, at ^ HALF, at)
                place = (2 * pr + lane // HALF) * rows + at * R1 + m1
                k_rows += [
                    k_pair[h * HS:(h + 1) * HS],
                    jnp.where(row0 & (place >= limit), MASKED, 0.0),
                ]
                v_rows += [v_pair[h * HS:(h + 1) * HS], jnp.where(row0, 1.0, 0.0)]
            keys.append(jnp.concatenate(k_rows, axis=0).astype(BF).T)
            values.append(jnp.concatenate(v_rows, axis=0).astype(BF))
        peak, out = attend(
            jnp.concatenate(keys, axis=0), jnp.concatenate(values, axis=1), q_wide
        )
        for h in range(heads):
            _, m1, a, _ = plans[h]
            col = slice((h // 2) * LANES, (h // 2 + 1) * LANES)
            o_h, lse = finish(peak[:, col], out[h * FP:(h + 1) * FP, col])
            z = jnp.concatenate([o_h, split(lse, LANES)], axis=0).astype(BF)
            put = mm_t(z, sel[a, pl.ds((h % 2) * square, square), :])
            spread[pl.ds(h * FP, HS), :] = put[:HS]
            lse = joined(put[HS:])
            lse = jnp.where(put[HS + 3:HS + 4] > 0.5, lse, MASKED)
            spread[pl.ds(h * FP + HS, 8), :] = jnp.broadcast_to(lse, (8, phase))
            two = plans[h][3][1]
            feat = pl.ds(h * HS, HS)
            lse = jnp.where(two == m1, lse, MASKED)
            ship(1, h, combine([
                (near_o[two, feat, :], near_l[two, pl.ds(h, 1), :]), (put[:HS], lse),
            ]))
        x_start(0, 1)

    def returned(heads_of):
        if heads_of == (0, 1):
            ret_copy(0, 2).wait_recv()
        else:
            ret_copy(heads_of[0]).wait_recv()
        for h in heads_of:
            fin_o[pl.ds(h * HS, HS), :] = ret[h, pl.ds(0, HS), :].astype(F32)
            fin_l[pl.ds(h, 1), :] = joined(ret[h, pl.ds(HS, TAIL), :].astype(F32))

    def conclude(heads_of):
        for h in heads_of:
            o0, m1 = plans[h][:2]
            feat = pl.ds(h * HS, HS)
            lse_w = spread[pl.ds(h * FP + HS, 1), :]
            ship(0, h, combine([
                (near_o[o0, feat, :], near_l[o0, pl.ds(h, 1), :]),
                (fin_o[feat, :], fin_l[pl.ds(h, 1), :]),
                (spread[pl.ds(h * FP, HS), :], jnp.where(m1 == o0, lse_w, MASKED)),
            ]))

    def guested(name, steps):
        @pl.when(is_guest)
        def _():
            with jax.named_scope(name):
                for step in steps:
                    step()

    guested("back01", [lambda: returned(early)])
    with jax.named_scope("conclude01"):
        conclude(early)
        x_start(1)
    for h in later:
        guested(f"back{h}", [lambda: returned((h,))])
        with jax.named_scope(f"conclude{h}"):
            conclude((h,))
            x_start(h)
    with jax.named_scope("x_fwd"):
        for group in range(direct):
            x_forward(group)

    passed = {x for _, x in onward}

    def x_finish(group):
        for x in range(1, n_sub):
            if x not in passed or group == direct:
                x_arrived(x, group)

    with jax.named_scope("x_wait"):
        x_finish(0)
        x_finish(1)

    every = [plan(i)[3] for i in range(n_sub * heads)]
    zeros_head = jnp.zeros((HS, phase), BF)
    with jax.named_scope("project_most"):
        for m in range(R1):
            parts = []
            for d in range(n_sub):
                for h in range(heads):
                    order = every[d * heads + h]
                    at = jnp.where(order[1] == m, 0, jnp.where(order[2] == m, 1, 2))
                    feat = pl.ds(h * HS, HS)
                    held = xl[d, feat, :] if h < heads // 2 else zeros_head
                    parts.append(jnp.where(order[0] == m, held, xg[d, at, feat, :]))
            near_o[m] = mm(wt[...], jnp.concatenate(parts, axis=0))
    with jax.named_scope("x_last"):
        x_finish(2)
        x_finish(direct)

    with jax.named_scope("project"):
        outs = []
        for m in range(R1):
            last = jnp.concatenate([
                jnp.where(
                    every[d * heads + h][0] == m, xl[d, pl.ds(h * HS, HS), :], zeros_head
                )
                for d in range(n_sub) for h in range(heads // 2, heads)
            ], axis=0)
            outs.append((near_o[m] + mm(wt_last[...], last)).astype(BF).astype(F32))
        for c in range(rows // (2 * square)):
            at = slice(c * LANES, (c + 1) * LANES)
            for odd in range(2):
                pieces = [
                    jnp.where(low, outs[2 * i + odd][:, at], outs[2 * i + 1 - odd][:, at])
                    for i in range(2)
                ]
                res = mm_t(jnp.concatenate(pieces, axis=1).astype(BF), perm[odd])
                first = (2 * c + odd) * square
                place = block0 + first + iota((1, square), 1)
                o_ref[:, first:first + square] = jnp.where(place < limit, res, 0.0).astype(BF)

    with jax.named_scope("drain"):
        def sent(ref, sem):
            pltpu.make_async_remote_copy(
                src_ref=ref, dst_ref=ref, send_sem=sem, recv_sem=sem,
                device_id={"sub": sub ^ 1}, device_id_type=MESH,
            ).wait_send()

        @pl.when(inner)
        def _():
            sent(wide, wide_send.at[0])

        @pl.when(jnp.logical_not(inner))
        def _():
            sent(wide.at[0], wide_send.at[0])

        @pl.when(is_host)
        def _():
            sent(mid.at[pl.ds(0, 2)], mid_send.at[0])
            sent(ret, ret_send.at[0])

        @pl.when(is_guest)
        def _():
            sent(mid.at[0], mid_send.at[0])
            q_copy().wait_send()

        sent(xg.at[pl.ds(0, n_sub - 1)], x_send.at[0])
        sent(xl.at[pl.ds(0, n_sub - 1)], x_send.at[1])


def local(n_seq, n_sub, q_heads, k_heads, v_heads, w_out, offsets, valid):
    rows, cols = q_heads.shape
    heads = cols // HS
    phase, strip = rows // R1, rows // R2
    assert heads == 4 and n_sub & (n_sub - 1) == 0 and n_seq % 2 == 0 and strip == HALF
    vmem = pl.BlockSpec(memory_space=pltpu.VMEM)
    pad = heads * FP
    return pl.pallas_call(
        functools.partial(kernel, n_seq, n_sub, heads),
        out_shape=jax.ShapeDtypeStruct((cols, rows), BF),
        in_specs=[pl.BlockSpec(memory_space=pl.ANY)] * 6,
        out_specs=vmem,
        scratch_shapes=[
            pltpu.SMEM(offsets.shape, I32),
            pltpu.SMEM(valid.shape, I32),
            pltpu.VMEM((cols, rows), BF),
            pltpu.VMEM((pad, rows), BF),
            pltpu.VMEM((pad, rows), BF),
            pltpu.VMEM(w_out.shape, BF),
            pltpu.VMEM((cols, w_out.shape[0]), BF),
            pltpu.VMEM((cols, n_sub * cols // 2), BF),
            pltpu.VMEM((2, 2 * LANES, 2 * LANES), BF),
            pltpu.VMEM((R1, 4 * LANES, LANES), BF),
            pltpu.VMEM((heads, rows, FP), BF),
            pltpu.VMEM((R1, pad, phase), BF),
            pltpu.VMEM((R1, cols, phase), BF),
            pltpu.VMEM((R1, cols, phase), BF),
            pltpu.VMEM((n_seq + 1, cols, LANES), BF),
            pltpu.VMEM((GROUP, heads, 2 * HS, phase), BF),
            pltpu.VMEM((cols, phase), BF),
            pltpu.VMEM((pad, 2 * phase), BF),
            pltpu.VMEM((heads, (GROUP - 1) * phase, FP), BF),
            pltpu.VMEM((pad, (GROUP - 1) * phase), BF),
            pltpu.VMEM((heads, HS + TAIL, phase), BF),
            pltpu.VMEM((cols, phase), F32),
            pltpu.VMEM((8, phase), F32),
            pltpu.VMEM((2, rows, phase), F32),
            pltpu.VMEM((R1, cols, phase), F32),
            pltpu.VMEM((R1, 8, phase), F32),
            pltpu.VMEM((pad, 2 * phase), F32),
            pltpu.VMEM((8, 2 * phase), F32),
            pltpu.VMEM((pad, phase), F32),
            pltpu.VMEM((n_sub, R1 - 1, cols, phase), BF),
            pltpu.VMEM((n_sub, cols, phase), BF),
            pltpu.SemaphoreType.DMA((1,)),
            pltpu.SemaphoreType.DMA((n_seq,)),
            pltpu.SemaphoreType.DMA((1,)),
            pltpu.SemaphoreType.DMA((3, 3)),
            pltpu.SemaphoreType.DMA((2,)),
            pltpu.SemaphoreType.DMA((1,)),
            pltpu.SemaphoreType.DMA((3,)),
            pltpu.SemaphoreType.DMA((2,)),
            pltpu.SemaphoreType.DMA((n_sub - 1, 4)),
            pltpu.SemaphoreType.DMA((6,)),
        ],
        compiler_params=pltpu.CompilerParams(
            collective_id=0, has_side_effects=True, vmem_limit_bytes=54784 * 1024
        ),
    )(q_heads.T, k_heads.T, v_heads.T, w_out, offsets, valid).T


def solution(mesh):
    spread = P(("slides", "seq"), "sub")
    return jax.shard_map(
        functools.partial(local, mesh.shape["seq"], mesh.shape["sub"]),
        mesh=mesh,
        in_specs=(spread, spread, spread, P(), P(), P("slides")),
        out_specs=spread,
        check_vma=False,
    )
```

```python
import functools

import jax
import jax.numpy as jnp
from jax import lax
from jax.experimental import pallas as pl
from jax.experimental.pallas import tpu as pltpu
from jax.sharding import PartitionSpec as P

HS = 48
FP = 64
TAIL = 8
GROUP = 4
R1 = 4
R2 = 16
LANES = 128
HALF = 64
MASKED = -1e30
MESH = pl.DeviceIdType.MESH
EXP_SCALE = HS ** (-0.5) * 1.4426950408889634
LOG2E = 1.4426950408889634
CONTRACT_LAST = (((1,), (1,)), ((), ()))
BF, F32, I32 = jnp.bfloat16, jnp.float32, jnp.int32


def iota(shape, dim):
    return lax.broadcasted_iota(I32, shape, dim)


def mm(a, b):
    return jnp.dot(a, b, preferred_element_type=F32)


def mm_t(a, b):
    return lax.dot_general(a, b, CONTRACT_LAST, preferred_element_type=F32)


def combine(parts):
    top = functools.reduce(jnp.maximum, [lse for _, lse in parts])
    weights = [jnp.exp2(lse - top) for _, lse in parts]
    scale = 1.0 / functools.reduce(jnp.add, weights)
    return functools.reduce(jnp.add, [o * (w * scale) for (o, _), w in zip(parts, weights)])


def kernel(
    n_seq, n_sub, heads,
    q_hbm, k_hbm, v_hbm, w_hbm, off_hbm, valid_hbm, o_ref,
    off_ref, valid_ref,
    q_ref, k_aug, v_aug, w_ref, wt,
    perm, sel, kr, pq, pk, pv, wide, mid,
    guest, mq, mkr, mv, ret, fin_o, fin_l,
    scores, near_o, near_l, mid_o, mid_m, spread, xg, xl,
    wide_send, wide_recv, mid_send, mid_recv, q_sem, ret_send, ret_recv, x_send, x_recv, in_sem,
):
    cols, rows = q_ref.shape
    phase = rows // R1
    strip = rows // R2
    square = 2 * LANES
    seq = lax.axis_index("seq")
    sub = lax.axis_index("sub")
    pos = lax.rem(seq, GROUP)
    group0 = seq - pos
    partner = pos ^ 1
    across = GROUP - 1 - pos
    far = across ^ 1
    is_host = (pos == 1) | (pos == 2)
    is_guest = jnp.logical_not(is_host)
    bits = [1 << b for b in reversed(range(n_sub.bit_length() - 1))]

    small = [
        pltpu.make_async_copy(off_hbm, off_ref, in_sem.at[4]),
        pltpu.make_async_copy(valid_hbm, valid_ref, in_sem.at[5]),
    ]
    for copy in small:
        copy.start()
    for i, (src, dst) in enumerate(((k_hbm, k_aug), (v_hbm, v_aug))):
        for h in range(heads):
            pltpu.make_async_copy(
                src.at[pl.ds(h * HS, HS), :], dst.at[pl.ds(h * FP, HS), :], in_sem.at[i]
            ).start()
    q_fetch = pltpu.make_async_copy(q_hbm, q_ref, in_sem.at[2])
    w_fetch = pltpu.make_async_copy(w_hbm, w_ref, in_sem.at[3])
    q_fetch.start()
    barrier = pltpu.get_barrier_semaphore()
    for step, there in ((1, seq < n_seq - 1), (-1, seq > 0)):
        @pl.when(there)
        def _():
            pl.semaphore_signal(
                barrier, inc=1, device_id={"seq": seq + step}, device_id_type=MESH
            )
    for x in range(1, n_sub):
        pl.semaphore_signal(barrier, inc=1, device_id={"sub": sub ^ x}, device_id_type=MESH)

    low = iota((1, LANES), 1) < HALF
    block0 = seq * rows

    def plan(head):
        o0, o1 = off_ref[0, head], off_ref[1, head]
        m1 = lax.rem(o1, R1)
        late = o0
        second = jnp.where(m1 == o0, lax.rem(o0 + 1, R1), m1)
        third = 0
        for m in reversed(range(R1 - 1)):
            third = jnp.where((late != m) & (second != m), m, third)
        return o0, m1, lax.div(o1, R1), (late, second, third, 6 - late - second - third)

    with jax.named_scope("consts"):
        tok, at = iota((square, square), 0), iota((square, square), 1)
        for odd in range(2):
            hit = tok == at % HALF * R1 + ((at // HALF) ^ odd)
            perm[odd] = jnp.where(hit, 1.0, 0.0).astype(BF)
        at_l, at_j = iota((square, LANES), 0), iota((square, LANES), 1)
        for a in range(R1):
            for half in range(2):
                hit = at_l == (at_j - half * HALF) * R1 + a
                sel[a, pl.ds(half * square, square), :] = jnp.where(hit, 1.0, 0.0).astype(BF)
        for copy in small:
            copy.wait()
        limit = valid_ref[0]
        plans = [plan(sub * heads + h) for h in range(heads)]
        tail_one = jnp.where(iota((FP - HS, square), 0) == 0, 1.0, 0.0).astype(BF)
        for h in range(heads):
            tail = pl.ds(h * FP + HS, FP - HS)
            for m in range(R1):
                pq[m, tail, :] = tail_one
            place = block0 + iota((FP - HS, rows), 1)
            first = iota((FP - HS, rows), 0) == 0
            v_aug[tail, :] = jnp.where(first, 1.0, 0.0).astype(BF)
            k_aug[tail, :] = jnp.where(first & (place >= limit), MASKED, 0.0).astype(BF)

    def permuted(lhs_of, store):
        for c in range(rows // (2 * square)):
            outs = [
                mm(lhs_of(pl.ds((2 * c + b) * square, square)), perm[b]) for b in range(2)
            ]
            for m in range(R1):
                half = slice((m // 2) * LANES, (m // 2 + 1) * LANES)
                even, odd = outs[0][:, half], outs[1][:, half]
                if m % 2:
                    even, odd = odd, even
                store(m, slice(c * LANES, (c + 1) * LANES), jnp.where(low, even, odd).astype(BF))

    with jax.named_scope("load"):
        for i, src in enumerate((k_hbm, v_hbm)):
            pltpu.make_async_copy(src, q_ref, in_sem.at[i]).wait()
        w_fetch.start()

        def store_kv(m, lanes, val):
            pk[m, :, lanes] = val[:cols]
            pv[m, :, lanes] = val[cols:]

        permuted(
            lambda t: jnp.concatenate(
                [ref[pl.ds(h * FP, HS), t] for ref in (k_aug, v_aug) for h in range(heads)], axis=0
            ),
            store_kv,
        )
        for h in range(heads):
            o0, m1, a, _ = plans[h]
            feat = pl.ds(h * HS, HS)
            mid[pos, h, pl.ds(0, HS), :] = pk[o0, feat, :]
            mid[pos, h, pl.ds(HS, HS), :] = pv[o0, feat, :]
            both = jnp.concatenate([pk[m1, feat, :], pv[m1, feat, :]], axis=1)
            wide[seq, feat, :] = mm(both, sel[a]).astype(BF)

    with jax.named_scope("barrier"):
        inner = (seq > 0) & (seq < n_seq - 1)

        @pl.when(inner)
        def _():
            pl.semaphore_wait(barrier, n_sub - 1 + 2)

        @pl.when(jnp.logical_not(inner))
        def _():
            pl.semaphore_wait(barrier, n_sub - 1 + 1)

    def wide_copy(origin, rightward):
        target = seq + 1 if rightward else seq - 1
        return pltpu.make_async_remote_copy(
            src_ref=wide.at[origin], dst_ref=wide.at[origin],
            send_sem=wide_send.at[0], recv_sem=wide_recv.at[origin],
            device_id={"seq": target}, device_id_type=MESH,
        )

    def wide_relay(dist):
        @pl.when(seq - dist >= 0)
        def _():
            wide_copy(seq - dist, True).wait_recv()

            @pl.when(seq < n_seq - 1)
            def _():
                wide_copy(seq - dist, True).start()

        @pl.when(seq + dist < n_seq)
        def _():
            wide_copy(seq + dist, False).wait_recv()

            @pl.when(seq > 0)
            def _():
                wide_copy(seq + dist, False).start()

    def mid_copy(origin, h, kind, count=1):
        ref = mid.at[origin, h if count == 1 else pl.ds(h, count)]
        return pltpu.make_async_remote_copy(
            src_ref=ref, dst_ref=ref,
            send_sem=mid_send.at[0], recv_sem=mid_recv.at[kind, max(h - 1, 0)],
            device_id={"seq": group0 + 1 + lax.rem(pos, 2)}, device_id_type=MESH,
        )

    def mid_arrived(origin, kind, heads_of):
        if heads_of == (0, 1):
            mid_copy(origin, 0, kind, 2).wait_recv()
        else:
            for h in heads_of:
                mid_copy(origin, h, kind).wait_recv()

    own_kind = jnp.where(is_host, 1, 0)

    def q_copy():
        return pltpu.make_async_remote_copy(
            src_ref=guest, dst_ref=guest, send_sem=q_sem.at[0], recv_sem=q_sem.at[1],
            device_id={"seq": group0 + partner}, device_id_type=MESH,
        )

    def ret_copy(h, count=1):
        ref = ret.at[h if count == 1 else pl.ds(h, count)]
        return pltpu.make_async_remote_copy(
            src_ref=ref, dst_ref=ref,
            send_sem=ret_send.at[0], recv_sem=ret_recv.at[max(h - 1, 0)],
            device_id={"seq": group0 + partner}, device_id_type=MESH,
        )

    def relay(heads_of):
        mid_arrived(partner, 0, heads_of)
        for h in heads_of:
            mid_copy(partner, h, 2).start()

    @pl.when(seq < n_seq - 1)
    def _():
        wide_copy(seq, True).start()

    @pl.when(seq > 0)
    def _():
        wide_copy(seq, False).start()

    for h in range(3):
        mid_copy(pos, h, own_kind).start()

    spans = {1: (0, 2), 2: (2, 1), 3: (3, 1)}
    direct = 3
    onward = [(bit, x) for bit in bits for x in range(1, n_sub) if not x % (2 * bit)]

    def x_ref(block, group, slab=None):
        if group:
            first, count = spans[group]
            return xl.at[block, pl.ds(first * HS, count * HS)]
        return xg.at[block] if slab is None else xg.at[block, slab - 1]

    def x_copy(ref, held, bit, group):
        return pltpu.make_async_remote_copy(
            src_ref=ref, dst_ref=ref, send_sem=x_send.at[1 if group else 0],
            recv_sem=x_recv.at[(held ^ bit) - 1, group],
            device_id={"sub": sub ^ bit}, device_id_type=MESH,
        )

    def x_start(group, slab=None):
        ref = x_ref(sub, group, slab)
        for bit in (reversed(range(1, n_sub)) if group == direct else bits):
            x_copy(ref, 0, bit, group).start()

    def x_arrived(x, group):
        x_copy(x_ref(sub ^ x, group), 0, x, group).wait_recv()

    def x_forward(group):
        waited = set()
        for bit, x in onward:
            if x not in waited:
                waited.add(x)
                x_arrived(x, group)
            x_copy(x_ref(sub ^ x, group), x, bit, group).start()

    with jax.named_scope("load_q"):
        q_fetch.wait()

        def store_q(m, lanes, val):
            for h in range(heads):
                pq[m, pl.ds(h * FP, HS), lanes] = val[h * HS:(h + 1) * HS]

        permuted(lambda t: q_ref[:, t], store_q)
        for h in range(heads):
            o0 = plans[h][0]
            mq[pl.ds(h * FP, FP), pl.ds(0, phase)] = pq[o0, pl.ds(h * FP, FP), :]

        @pl.when(is_guest)
        def _():
            for h in range(heads):
                guest[pl.ds(h * HS, HS), :] = pq[plans[h][0], pl.ds(h * FP, HS), :]

    @pl.when(is_guest)
    def _():
        mid_copy(pos, 3, own_kind).start()
        q_copy().start()

    with jax.named_scope("prep"):
        for h in range(heads):
            kr[h] = k_aug[pl.ds(h * FP, FP), :].T

    def attend(keys, values, queries, before=None):
        scores = mm(keys, queries)
        peak = jnp.max(scores, axis=0, keepdims=True)
        if before is not None:
            peak = jnp.maximum(peak, before)
        probs = jnp.exp2((scores - peak) * EXP_SCALE).astype(BF)
        return peak, mm(values, probs)

    def finish(peak, out):
        mass = out[HS:HS + 1]
        return out[:HS] * (1.0 / mass), peak * EXP_SCALE + jnp.log(mass) * LOG2E

    def pipeline(jobs, pieces, keys, queries, values, done):
        def score(i, c, peak):
            part = mm(keys(jobs[i], c), queries(jobs[i]))
            scores[i % 2, pl.ds(c * phase, phase), :] = part
            top = jnp.max(part, axis=0, keepdims=True)
            return top if peak is None else jnp.maximum(peak, top)

        peak = None
        for c in range(pieces):
            peak = score(0, c, peak)
        for i, job in enumerate(jobs):
            ahead = acc = None
            for c in range(pieces):
                if i + 1 < len(jobs):
                    ahead = score(i + 1, c, ahead)
                part = scores[i % 2, pl.ds(c * phase, phase), :]
                probs = jnp.exp2((part - peak) * EXP_SCALE).astype(BF)
                out = mm(values(job, c), probs)
                acc = out if acc is None else acc + out
            done(i, job, peak, acc)
            peak = ahead

    def near_done(i, job, peak, acc):
        m, h = job
        out, lse = finish(peak, acc)
        near_o[m, pl.ds(h * HS, HS), :] = out
        near_l[m, pl.ds(h, 1), :] = lse
        for when, mine in ((6, lax.rem(sub, 2) == 1), (8, lax.rem(sub, 2) == 0)):
            if i == when:
                @pl.when(mine)
                def _():
                    wide_relay(1)

                    @pl.when(is_host)
                    def _():
                        mid_copy(pos, 3, own_kind).start()

    with jax.named_scope("near"):
        pipeline(
            [(m, h) for m in range(R1) for h in range(heads)],
            rows // phase,
            lambda job, c: kr[job[1], pl.ds(c * phase, phase), :],
            lambda job: pq[job[0], pl.ds(job[1] * FP, FP), :],
            lambda job, c: v_aug[pl.ds(job[1] * FP, FP), pl.ds(c * phase, phase)],
            near_done,
        )

    def ship(slab, h, val):
        at = pl.ds(h * HS, HS)
        if slab:
            xg[sub, slab - 1, at, :] = val.astype(BF)
        else:
            xl[sub, at, :] = val.astype(BF)

    with jax.named_scope("ship_near"):
        for slab in (2, 3):
            for h in range(heads):
                ship(slab, h, near_o[plans[h][3][slab], pl.ds(h * HS, HS), :])
            x_start(0, slab)

    ones_tail = jnp.where(iota((FP - HS, phase), 0) == 0, 1.0, 0.0).astype(BF)

    def split(lse, width, count=FP - HS):
        top = jnp.floor(lse * 0.25) * 4.0
        rest = lse - top
        middle = jnp.floor(rest * 64.0) * (1.0 / 64.0)
        r = iota((count, width), 0)
        low_part = jnp.where(r == 2, rest - middle, jnp.where(r == 3, 1.0, 0.0))
        return jnp.where(r == 0, top, jnp.where(r == 1, middle, low_part))

    def joined(rows_of):
        return rows_of[0:1] + rows_of[1:2] + rows_of[2:3]

    def mid_kv(origin, h):
        o0 = plans[h][0]
        lane = iota((FP - HS, phase), 1)
        at = jnp.where(lax.rem(o0, 2) == 1, lane ^ HALF, lane)
        place = (group0 + origin) * rows + at * R1 + o0
        dead = (iota((FP - HS, phase), 0) == 0) & (place >= limit)
        dead = jnp.where(dead, MASKED, 0.0).astype(BF)
        return (
            jnp.concatenate([mid[origin, h, pl.ds(0, HS), :], dead], axis=0).T,
            jnp.concatenate([mid[origin, h, pl.ds(HS, HS), :], ones_tail], axis=0),
        )

    def mid_stage(origin, slot):
        for h in range(heads):
            at = pl.ds(slot * phase, phase)
            mkr[h, at, :], mv[pl.ds(h * FP, FP), at] = mid_kv(origin, h)

    def mid_pass():
        def done(i, job, peak, acc):
            h, t = job
            at = pl.ds(t * phase, phase)
            mid_m[pl.ds(h, 1), at] = peak
            mid_o[pl.ds(h * FP, FP), at] = acc

        pipeline(
            [(h, t) for h in range(heads) for t in range(2)],
            GROUP - 1,
            lambda job, c: mkr[job[0], pl.ds(c * phase, phase), :],
            lambda job: mq[pl.ds(job[0] * FP, FP), pl.ds(job[1] * phase, phase)],
            lambda job, c: mv[pl.ds(job[0] * FP, FP), pl.ds(c * phase, phase)],
            done,
        )

    def mid_step(origin, heads_of):
        staged = [mid_kv(origin, h) for h in heads_of]
        scored = [
            mm(keys, mq[pl.ds(h * FP, FP), :]) for h, (keys, _) in zip(heads_of, staged)
        ]
        fore = [(mid_m[pl.ds(h, 1), :], mid_o[pl.ds(h * FP, FP), :]) for h in heads_of]
        done = []
        for score, (_, vals), (before, _) in zip(scored, staged, fore):
            peak = jnp.maximum(jnp.max(score, axis=0, keepdims=True), before)
            probs = jnp.exp2((score - peak) * EXP_SCALE).astype(BF)
            done.append((peak, mm(vals, probs)))
        return [
            (peak, out + old * jnp.exp2((before - peak) * EXP_SCALE))
            for (peak, out), (before, old) in zip(done, fore)
        ]

    def hosted(name, steps):
        @pl.when(is_host)
        def _():
            with jax.named_scope(name):
                for step in steps:
                    step()

    def guest_queries():
        q_copy().wait_recv()
        for h in range(heads):
            at = pl.ds(phase, phase)
            mq[pl.ds(h * FP, HS), at] = guest[pl.ds(h * HS, HS), :]
            mq[pl.ds(h * FP + HS, FP - HS), at] = tail_one

    early, later = (0, 1), (2, 3)
    hosted("relay", [lambda: relay(early), lambda: relay(later)])
    with jax.named_scope("wide_relay2"):
        wide_relay(2)
    hosted("mid_stage", [
        lambda: mid_stage(pos, 0),
        lambda: mid_stage(partner, 1),
        lambda: mid_arrived(across, 1, early),
        lambda: mid_arrived(across, 1, later),
        lambda: mid_stage(across, 2),
    ])
    hosted("guest_q", [guest_queries])
    hosted("mid_pass", [mid_pass])
    def mid_last(heads_of):
        mid_arrived(far, 2, heads_of)
        done = mid_step(far, heads_of)
        for h, (peak, out) in zip(heads_of, done):
            o, lse = finish(peak, out)
            feat = pl.ds(h * FP, HS)
            ret[h, pl.ds(0, HS), :] = o[:, phase:].astype(BF)
            ret[h, pl.ds(HS, TAIL), :] = split(lse[:, phase:], phase, TAIL).astype(BF)
            ret_copy(h).start()
            fin_o[pl.ds(h * HS, HS), :] = o[:, :phase]
            fin_l[pl.ds(h, 1), :] = lse[:, :phase]

    hosted("mid_last01", [lambda: mid_last(early)])
    hosted("mid_last2", [lambda: mid_last((2,))])
    hosted("mid_last3", [lambda: mid_last((3,))])
    with jax.named_scope("weights"):
        w_fetch.wait()
        for s in range(n_sub):
            @pl.when(sub == s)
            def _():
                mine = slice(s * cols, (s + 1) * cols)
                wt[...] = w_ref[:, mine].T
    with jax.named_scope("wide_relay3"):
        for dist in range(3, n_seq):
            wide_relay(dist)

    with jax.named_scope("wide"):
        q_rows = []
        for h in range(heads):
            _, m1, a, _ = plans[h]
            q_h = mm(pq[m1, pl.ds(h * FP, FP), :], sel[a, pl.ds((h % 2) * square, square), :])
            zero = jnp.zeros((FP, LANES), BF)
            q_h = q_h.astype(BF)
            q_rows.append(jnp.concatenate([q_h, zero] if h < 2 else [zero, q_h], axis=1))
        q_wide = jnp.concatenate(q_rows, axis=0)
        keys, values = [], []
        zeros_tail = jnp.zeros((FP - HS - 8, LANES), F32)
        for pr in range(n_seq // 2):
            one, two = [wide[2 * pr + i].astype(F32) for i in range(2)]
            k_pair = jnp.where(low, one, pltpu.roll(two, HALF, 1))
            v_pair = jnp.where(low, pltpu.roll(one, HALF, 1), two)
            k_rows, v_rows = [], []
            for h in range(heads):
                _, m1, a, _ = plans[h]
                lane = iota((FP - HS, LANES), 1)
                row0 = iota((FP - HS, LANES), 0) == 0
                at = lane % HALF * R1 + a
                at = jnp.where(lax.rem(m1, 2) == 1, at ^ HALF, at)
                place = (2 * pr + lane // HALF) * rows + at * R1 + m1
                k_rows += [
                    k_pair[h * HS:(h + 1) * HS],
                    jnp.where(row0 & (place >= limit), MASKED, 0.0),
                ]
                v_rows += [v_pair[h * HS:(h + 1) * HS], jnp.where(row0, 1.0, 0.0)]
            keys.append(jnp.concatenate(k_rows, axis=0).astype(BF).T)
            values.append(jnp.concatenate(v_rows, axis=0).astype(BF))
        peak, out = attend(
            jnp.concatenate(keys, axis=0), jnp.concatenate(values, axis=1), q_wide
        )
        for h in range(heads):
            _, m1, a, _ = plans[h]
            col = slice((h // 2) * LANES, (h // 2 + 1) * LANES)
            o_h, lse = finish(peak[:, col], out[h * FP:(h + 1) * FP, col])
            z = jnp.concatenate([o_h, split(lse, LANES)], axis=0).astype(BF)
            put = mm_t(z, sel[a, pl.ds((h % 2) * square, square), :])
            spread[pl.ds(h * FP, HS), :] = put[:HS]
            lse = joined(put[HS:])
            lse = jnp.where(put[HS + 3:HS + 4] > 0.5, lse, MASKED)
            spread[pl.ds(h * FP + HS, 8), :] = jnp.broadcast_to(lse, (8, phase))
            two = plans[h][3][1]
            feat = pl.ds(h * HS, HS)
            lse = jnp.where(two == m1, lse, MASKED)
            ship(1, h, combine([
                (near_o[two, feat, :], near_l[two, pl.ds(h, 1), :]), (put[:HS], lse),
            ]))
        x_start(0, 1)

    def returned(heads_of):
        if heads_of == (0, 1):
            ret_copy(0, 2).wait_recv()
        else:
            ret_copy(heads_of[0]).wait_recv()
        for h in heads_of:
            fin_o[pl.ds(h * HS, HS), :] = ret[h, pl.ds(0, HS), :].astype(F32)
            fin_l[pl.ds(h, 1), :] = joined(ret[h, pl.ds(HS, TAIL), :].astype(F32))

    def conclude(heads_of):
        for h in heads_of:
            o0, m1 = plans[h][:2]
            feat = pl.ds(h * HS, HS)
            lse_w = spread[pl.ds(h * FP + HS, 1), :]
            ship(0, h, combine([
                (near_o[o0, feat, :], near_l[o0, pl.ds(h, 1), :]),
                (fin_o[feat, :], fin_l[pl.ds(h, 1), :]),
                (spread[pl.ds(h * FP, HS), :], jnp.where(m1 == o0, lse_w, MASKED)),
            ]))

    def guested(name, steps):
        @pl.when(is_guest)
        def _():
            with jax.named_scope(name):
                for step in steps:
                    step()

    guested("back01", [lambda: returned(early)])
    with jax.named_scope("conclude01"):
        conclude(early)
        x_start(1)
    for h in later:
        guested(f"back{h}", [lambda: returned((h,))])
        with jax.named_scope(f"conclude{h}"):
            conclude((h,))
            x_start(h)
    passed = {x for _, x in onward}

    def x_finish(group):
        for x in range(1, n_sub):
            if x not in passed or group == direct:
                x_arrived(x, group)

    def x_pass_late(parity):
        @pl.when(lax.rem(sub, 2) == parity)
        def _():
            for group in range(1, direct):
                x_forward(group)

    with jax.named_scope("x_fwd"):
        x_forward(0)
        x_pass_late(1)
        x_finish(0)

    every = [plan(i)[3] for i in range(n_sub * heads)]
    zeros_head = jnp.zeros((HS, phase), BF)
    with jax.named_scope("project_most"):
        for m in range(R1):
            parts = []
            for d in range(n_sub):
                for h in range(heads):
                    order = every[d * heads + h]
                    at = jnp.where(order[1] == m, 0, jnp.where(order[2] == m, 1, 2))
                    feat = pl.ds(h * HS, HS)
                    parts.append(jnp.where(order[0] == m, zeros_head, xg[d, at, feat, :]))
            near_o[m] = mm(wt[...], jnp.concatenate(parts, axis=0))
    with jax.named_scope("x_last"):
        x_pass_late(0)
        for group in range(1, direct + 1):
            x_finish(group)

    with jax.named_scope("project"):
        outs = []
        for m in range(R1):
            last = jnp.concatenate([
                jnp.where(
                    every[d * heads + h][0] == m, xl[d, pl.ds(h * HS, HS), :], zeros_head
                )
                for d in range(n_sub) for h in range(heads)
            ], axis=0)
            outs.append((near_o[m] + mm(wt[...], last)).astype(BF).astype(F32))
        for c in range(rows // (2 * square)):
            at = slice(c * LANES, (c + 1) * LANES)
            for odd in range(2):
                pieces = [
                    jnp.where(low, outs[2 * i + odd][:, at], outs[2 * i + 1 - odd][:, at])
                    for i in range(2)
                ]
                res = mm_t(jnp.concatenate(pieces, axis=1).astype(BF), perm[odd])
                first = (2 * c + odd) * square
                place = block0 + first + iota((1, square), 1)
                o_ref[:, first:first + square] = jnp.where(place < limit, res, 0.0).astype(BF)

    with jax.named_scope("drain"):
        def sent(ref, sem):
            pltpu.make_async_remote_copy(
                src_ref=ref, dst_ref=ref, send_sem=sem, recv_sem=sem,
                device_id={"sub": sub ^ 1}, device_id_type=MESH,
            ).wait_send()

        @pl.when(inner)
        def _():
            sent(wide, wide_send.at[0])

        @pl.when(jnp.logical_not(inner))
        def _():
            sent(wide.at[0], wide_send.at[0])

        @pl.when(is_host)
        def _():
            sent(mid.at[pl.ds(0, 2)], mid_send.at[0])
            sent(ret, ret_send.at[0])

        @pl.when(is_guest)
        def _():
            sent(mid.at[0], mid_send.at[0])
            q_copy().wait_send()

        sent(xg.at[pl.ds(0, n_sub - 1)], x_send.at[0])
        sent(xl.at[pl.ds(0, n_sub - 1)], x_send.at[1])


def local(n_seq, n_sub, q_heads, k_heads, v_heads, w_out, offsets, valid):
    rows, cols = q_heads.shape
    heads = cols // HS
    phase, strip = rows // R1, rows // R2
    assert heads == 4 and n_sub & (n_sub - 1) == 0 and n_seq % 2 == 0 and strip == HALF
    vmem = pl.BlockSpec(memory_space=pltpu.VMEM)
    pad = heads * FP
    return pl.pallas_call(
        functools.partial(kernel, n_seq, n_sub, heads),
        out_shape=jax.ShapeDtypeStruct((cols, rows), BF),
        in_specs=[pl.BlockSpec(memory_space=pl.ANY)] * 6,
        out_specs=vmem,
        scratch_shapes=[
            pltpu.SMEM(offsets.shape, I32),
            pltpu.SMEM(valid.shape, I32),
            pltpu.VMEM((cols, rows), BF),
            pltpu.VMEM((pad, rows), BF),
            pltpu.VMEM((pad, rows), BF),
            pltpu.VMEM(w_out.shape, BF),
            pltpu.VMEM((cols, w_out.shape[0]), BF),
            pltpu.VMEM((2, 2 * LANES, 2 * LANES), BF),
            pltpu.VMEM((R1, 4 * LANES, LANES), BF),
            pltpu.VMEM((heads, rows, FP), BF),
            pltpu.VMEM((R1, pad, phase), BF),
            pltpu.VMEM((R1, cols, phase), BF),
            pltpu.VMEM((R1, cols, phase), BF),
            pltpu.VMEM((n_seq + 1, cols, LANES), BF),
            pltpu.VMEM((GROUP, heads, 2 * HS, phase), BF),
            pltpu.VMEM((cols, phase), BF),
            pltpu.VMEM((pad, 2 * phase), BF),
            pltpu.VMEM((heads, (GROUP - 1) * phase, FP), BF),
            pltpu.VMEM((pad, (GROUP - 1) * phase), BF),
            pltpu.VMEM((heads, HS + TAIL, phase), BF),
            pltpu.VMEM((cols, phase), F32),
            pltpu.VMEM((8, phase), F32),
            pltpu.VMEM((2, rows, phase), F32),
            pltpu.VMEM((R1, cols, phase), F32),
            pltpu.VMEM((R1, 8, phase), F32),
            pltpu.VMEM((pad, 2 * phase), F32),
            pltpu.VMEM((8, 2 * phase), F32),
            pltpu.VMEM((pad, phase), F32),
            pltpu.VMEM((n_sub, R1 - 1, cols, phase), BF),
            pltpu.VMEM((n_sub, cols, phase), BF),
            pltpu.SemaphoreType.DMA((1,)),
            pltpu.SemaphoreType.DMA((n_seq,)),
            pltpu.SemaphoreType.DMA((1,)),
            pltpu.SemaphoreType.DMA((3, 3)),
            pltpu.SemaphoreType.DMA((2,)),
            pltpu.SemaphoreType.DMA((1,)),
            pltpu.SemaphoreType.DMA((3,)),
            pltpu.SemaphoreType.DMA((2,)),
            pltpu.SemaphoreType.DMA((n_sub - 1, 4)),
            pltpu.SemaphoreType.DMA((6,)),
        ],
        compiler_params=pltpu.CompilerParams(
            collective_id=0, has_side_effects=True, vmem_limit_bytes=54784 * 1024
        ),
    )(q_heads.T, k_heads.T, v_heads.T, w_out, offsets, valid).T


def solution(mesh):
    spread = P(("slides", "seq"), "sub")
    return jax.shard_map(
        functools.partial(local, mesh.shape["seq"], mesh.shape["sub"]),
        mesh=mesh,
        in_specs=(spread, spread, spread, P(), P(), P("slides")),
        out_specs=spread,
        check_vma=False,
    )
```
